256 devices in a mesh: member: 4 (over x), dom: 64 (over y, z, core).
Axes of the slice: x: 4, y: 4, z: 8, core: 2. Of those that a mesh axis runs over, the one named last changes fastest.
Arguments:
- acoustic_perturbation: float32 [4, 32, 65536], P('member', None, 'dom'), may hold values from -8 to 8
- prior_acoustic_state: float32 [4, 32, 65536], P('member', None, 'dom'), may hold values from -8 to 8
- thermal_anomaly: float32 [4, 32, 65536], P('member', None, 'dom'), may hold values from -8 to 8
- model_parameters: float32 [4, 4], P('member'), may hold values from 0.5 to 1.5
- crossing_velocity: float32 [32, 196608], P(None, 'dom'), may hold values from -3 to 3
- face_extent: float32 [196608], P('dom'), may hold values from 0.1 to 0.4
- face_metric_factor: float32 [196608], P('dom'), may hold values from 0.01 to 0.06
- reciprocal_polygon_surface: float32 [65536], P('dom'), may hold values from 0.5 to 2
- owned_totals: int32 [64], P('dom'), may hold values from 768 to 1024, as said below
- export_lists: int32 [64, 6, 128], P('dom'), may hold values from 0 to 1024, as said below
- face_neighbour_pair: int32 [2, 196608], P(None, 'dom'), may hold values from 0 to 1792, as said below
- polygon_side_lookup: int32 [6, 65536], P(None, 'dom'), may hold values from 0 to 3072, as said below
Outputs:
- pressure_out: float32 [4, 32, 65536], P('member', None, 'dom')
- temperature_out: float32 [4, 32, 65536], P('member', None, 'dom')
- ensemble_mean: float32 [32, 65536], P(None, 'dom')
The draws below stay inside these ranges and needn't reach their ends.
Inputs may be any that keep to these rules, and one draw needn't show every extreme that they name: The first owned_totals[p] cell slots of partition p are its cells, the rest unused; some partition has 1024. Row export_lists[p, b] lists owned cells of partition p sent to partition (p + offsets[b]) mod 64; filled entries first, then 1024 in the empty slots; at least 64 filled entries a row; in every draw some partition receives 128 filled entries in all 6 of its rows. `face_neighbour_pair`: edge 3 i + j of partition p starts at owned cell i and ends at another owned cell or at halo column 1024 + b * 128 + k whose slot k is filled in the sender's row b; edges of unused cells have both ends at 1792. `polygon_side_lookup`: the local edges with an end at each owned cell, 3072 in empty slots; unused cells have only empty slots.
All inputs are finite; a program needn't handle non-finite values.
Results may differ from the reference program's by a relative error of at most 0.0001.
Values sent between devices are 32-bit elements; how exact they have to be, the bound alone decides.
A program may use at most 64 MiB of HBM per device.

```python
import math
import jax
import jax.numpy as jnp

DOMAIN_CAPACITY = 1024
VERTICAL_LAYERS = 32
HB = 128
NB = 6
MAXE = 6
STEPS = 2
NS = 3
E_DEV = 3072
CELLS = 65536
EDGES = 196608
MEMBERS = 4
N_DOM = 64


def neighbour_offsets_drawn(count):
    return [(block_number // 2 + 1) * (1 - 2 * (block_number % 2)) for block_number in range(count)]


def mesh_tables(key):
    keys = jax.random.split(jax.random.fold_in(key, 7), 9)
    cell_counts = jax.random.randint(keys[0], (N_DOM,), 3 * DOMAIN_CAPACITY // 4, DOMAIN_CAPACITY + 1)
    full_part = jax.random.randint(keys[1], (), 0, N_DOM)
    cell_counts = cell_counts.at[full_part].set(DOMAIN_CAPACITY).astype(jnp.int32)
    offsets = jnp.array(neighbour_offsets_drawn(NB), jnp.int32)
    block_ids = jnp.arange(NB, dtype=jnp.int32)
    filled = jax.random.randint(keys[2], (N_DOM, NB), HB // 2, HB + 1)
    receiver = jax.random.randint(keys[3], (), 0, N_DOM)
    senders = (receiver - offsets) % N_DOM
    filled = filled.at[senders, block_ids].set(HB)
    slot_ids = jnp.arange(HB, dtype=jnp.int32)
    send_raw = jax.random.randint(keys[4], (N_DOM, NB, HB), 0, cell_counts[:, None, None])
    send_table = jnp.where(slot_ids[None, None, :] < filled[:, :, None], send_raw, DOMAIN_CAPACITY).astype(jnp.int32)
    part_ids = jnp.arange(N_DOM, dtype=jnp.int32)
    filled_in = filled[(part_ids[:, None] - offsets[None, :]) % N_DOM, block_ids[None, :]]
    cell_ids = jnp.arange(DOMAIN_CAPACITY, dtype=jnp.int32)
    halo_flag = jax.random.randint(keys[5], (N_DOM, DOMAIN_CAPACITY, 3), 0, 2)
    shifts = jax.random.randint(keys[6], (N_DOM, 3), 1, cell_counts[:, None])
    local_end = (cell_ids[None, :, None] + shifts[:, None, :]) % cell_counts[:, None, None]
    halo_block = jax.random.randint(keys[7], (N_DOM, DOMAIN_CAPACITY, 3), 0, NB)
    block_fill = filled_in[part_ids[:, None, None], halo_block]
    halo_slot = jax.random.randint(keys[8], (N_DOM, DOMAIN_CAPACITY, 3), 0, block_fill)
    halo_end = DOMAIN_CAPACITY + halo_block * HB + halo_slot
    valid = cell_ids[None, :, None] < cell_counts[:, None, None]
    zero_col = DOMAIN_CAPACITY + NB * HB
    start_cell = jnp.where(valid, cell_ids[None, :, None] + 0 * halo_flag, zero_col)
    end_cell = jnp.where(valid, jnp.where(halo_flag == 1, halo_end, local_end), zero_col)
    edge_table = jnp.stack([start_cell.reshape(N_DOM, E_DEV), end_cell.reshape(N_DOM, E_DEV)]).reshape(2, EDGES).astype(jnp.int32)
    side_ids = jnp.arange(3, dtype=jnp.int32)
    outgoing = jnp.where(valid, 3 * cell_ids[None, :, None] + side_ids[None, None, :], E_DEV)
    source = (cell_ids[None, :, None] - shifts[:, None, :]) % cell_counts[:, None, None]
    source_flag = jnp.take_along_axis(halo_flag, source, axis=1)
    incoming = jnp.where(valid & (source_flag == 0), 3 * source + side_ids[None, None, :], E_DEV)
    incidence = jnp.concatenate([outgoing, incoming], axis=2)
    incidence = jnp.transpose(incidence, (2, 0, 1)).reshape(MAXE, CELLS).astype(jnp.int32)
    return (cell_counts, send_table, edge_table, incidence)


def draw_owned_totals(key, part):
    return mesh_tables(key)[0]


def draw_export_lists(key, part):
    return mesh_tables(key)[1]


def draw_face_neighbour_pair(key, part):
    return mesh_tables(key)[2]


def draw_polygon_side_lookup(key, part):
    return mesh_tables(key)[3]


def regional_field(key):
    keys = jax.random.split(key, 2)
    region = 1.5 * jax.random.normal(keys[0], (MEMBERS, 1, N_DOM, 1), jnp.float32)
    noise = jax.random.normal(keys[1], (MEMBERS, VERTICAL_LAYERS, N_DOM, DOMAIN_CAPACITY), jnp.float32)
    return jnp.clip(region + noise, -8.0, 8.0).reshape(MEMBERS, VERTICAL_LAYERS, CELLS)


def draw_acoustic_perturbation(key, part):
    return regional_field(jax.random.fold_in(key, 11))


def draw_prior_acoustic_state(key, part):
    base = regional_field(jax.random.fold_in(key, 11))
    jitter = 0.3 * jax.random.normal(jax.random.fold_in(key, 12), (MEMBERS, VERTICAL_LAYERS, CELLS), jnp.float32)
    return jnp.clip(base + jitter, -8.0, 8.0)


def draw_thermal_anomaly(key, part):
    return regional_field(jax.random.fold_in(key, 13))


def levels(rng, dims, shards, smallest, top_value):
    level, own = 1.0, jax.random.fold_in(rng, 6)
    for dim, parts in shards:
        steps = jnp.exp(jax.random.uniform(jax.random.fold_in(own, dim), (parts,), jnp.float32, smallest / len(shards), top_value / len(shards)))
        level = level * jnp.repeat(steps, dims[dim] // parts).reshape([-1 if axis == dim else 1 for axis in range(len(dims))])
    return level


def centred(stream_key, extent, deviation, most, shards=(), held_as=jnp.bfloat16):
    factor_of = levels(stream_key, extent, shards, -0.22, 0.18) if shards else 1.0
    values = jax.random.normal(stream_key, extent, jnp.float32) * deviation * factor_of
    return jnp.minimum(jnp.maximum(values, -most), most).astype(held_as)


def setup_inputs(seed: int = 0) -> dict:
    key_list = jax.random.split(jax.random.key(seed), 13)
    acoustic_perturbation = draw_acoustic_perturbation(jax.random.fold_in(key_list[12], 71), 0)
    prior_acoustic_state = draw_prior_acoustic_state(jax.random.fold_in(key_list[12], 71), 0)
    thermal_anomaly = draw_thermal_anomaly(jax.random.fold_in(key_list[12], 71), 0)
    model_parameters = jnp.clip(0.5 + 1.0 * jax.random.uniform(key_list[3], (MEMBERS, 4), jnp.float32) ** levels(key_list[3], (MEMBERS, 4), ((0, 4),), -0.2, 0.2), 0.5, 1.5)
    crossing_velocity = centred(key_list[4], (VERTICAL_LAYERS, EDGES), 0.5, 3.0, ((1, 64),), jnp.float32)
    face_extent = jnp.clip(jnp.exp(math.log(0.4) - 1.3862944 * jax.random.uniform(key_list[5], (EDGES,), jnp.float32) ** levels(key_list[5], (EDGES,), ((0, 64),), -0.2, 0.2)), 0.1, 0.4)
    face_metric_factor = jnp.clip(jnp.exp(math.log(0.06) - 1.7917595 * jax.random.uniform(key_list[6], (EDGES,), jnp.float32) ** levels(key_list[6], (EDGES,), ((0, 64),), -0.2, 0.2)), 0.01, 0.06)
    reciprocal_polygon_surface = jnp.clip(jnp.exp(math.log(2.0) - 1.3862944 * jax.random.uniform(key_list[7], (CELLS,), jnp.float32) ** levels(key_list[7], (CELLS,), ((0, 64),), -0.2, 0.2)), 0.5, 2.0)
    owned_totals = draw_owned_totals(jax.random.fold_in(key_list[12], 71), 0)
    export_lists = draw_export_lists(jax.random.fold_in(key_list[12], 71), 0)
    face_neighbour_pair = draw_face_neighbour_pair(jax.random.fold_in(key_list[12], 71), 0)
    polygon_side_lookup = draw_polygon_side_lookup(jax.random.fold_in(key_list[12], 71), 0)
    return dict(acoustic_perturbation=acoustic_perturbation, prior_acoustic_state=prior_acoustic_state, thermal_anomaly=thermal_anomaly, model_parameters=model_parameters, crossing_velocity=crossing_velocity, face_extent=face_extent, face_metric_factor=face_metric_factor, reciprocal_polygon_surface=reciprocal_polygon_surface, owned_totals=owned_totals, export_lists=export_lists, face_neighbour_pair=face_neighbour_pair, polygon_side_lookup=polygon_side_lookup)


time_step = 0.25


def neighbour_offsets(count):
    return [(block_number // 2 + 1) * (1 - 2 * (block_number % 2)) for block_number in range(count)]


def extend_all(fields, export_lists):
    row_count = fields.shape[0]
    zero_column = jnp.zeros((row_count, N_DOM, 1), jnp.float32)
    padded_fields = jnp.concatenate([fields, zero_column], axis=2)
    pieces = [fields]
    for block_number, offset in enumerate(neighbour_offsets(NB)):
        sources = ((jnp.arange(N_DOM, dtype=jnp.int32) - offset) % N_DOM).astype(jnp.int32)
        chosen = export_lists[sources, block_number, :]
        pieces.append(jnp.take_along_axis(padded_fields[:, sources, :], chosen[None], axis=2))
    pieces.append(zero_column)
    return jnp.concatenate(pieces, axis=2)


def at_cells(extended, cell_list):
    return jnp.take_along_axis(extended, cell_list[None], axis=2)


def divergence_all(fluxes, polygon_side_lookup, edge_sign):
    padded_flux = jnp.concatenate([fluxes, jnp.zeros((fluxes.shape[0], N_DOM, 1), jnp.float32)], axis=2)
    summed = jnp.zeros((fluxes.shape[0], N_DOM, DOMAIN_CAPACITY), jnp.float32)
    for corner in range(MAXE):
        summed = summed + edge_sign[corner][None] * at_cells(padded_flux, polygon_side_lookup[corner])
    return summed


def reference(acoustic_perturbation, prior_acoustic_state, thermal_anomaly, model_parameters, crossing_velocity, face_extent, face_metric_factor, reciprocal_polygon_surface, owned_totals, export_lists, face_neighbour_pair, polygon_side_lookup):
    wind = crossing_velocity.reshape(VERTICAL_LAYERS, N_DOM, E_DEV)
    lengths = face_extent.reshape(N_DOM, E_DEV)[None]
    weights = face_metric_factor.reshape(N_DOM, E_DEV)[None]
    inverse = reciprocal_polygon_surface.reshape(N_DOM, DOMAIN_CAPACITY)[None]
    ends = face_neighbour_pair.reshape(2, N_DOM, E_DEV)
    incident = polygon_side_lookup.reshape(MAXE, N_DOM, DOMAIN_CAPACITY)
    cell_ids = jnp.arange(DOMAIN_CAPACITY, dtype=jnp.int32)
    owned = (cell_ids[None, :] < owned_totals[:, None])[None]
    cell_area = jnp.where(owned, 1.0 / inverse, jnp.float32(0.0))
    starts_padded = jnp.concatenate([ends[0], jnp.full((N_DOM, 1), -1, jnp.int32)], axis=1)
    edge_sign = jnp.stack([
        jnp.where(jnp.take_along_axis(starts_padded, incident[corner], axis=1) == cell_ids[None, :], jnp.float32(1.0), jnp.float32(-1.0))
        for corner in range(MAXE)])
    press_list, temp_list = [], []
    for perturbed_run in range(MEMBERS):
        speed = model_parameters[perturbed_run, 0]
        kappa = 0.5 * model_parameters[perturbed_run, 1]
        mixing = 0.6 * model_parameters[perturbed_run, 2]
        couple = model_parameters[perturbed_run, 3]
        current = acoustic_perturbation[perturbed_run].reshape(VERTICAL_LAYERS, N_DOM, DOMAIN_CAPACITY)
        previous = prior_acoustic_state[perturbed_run].reshape(VERTICAL_LAYERS, N_DOM, DOMAIN_CAPACITY)
        scalar_quantity = thermal_anomaly[perturbed_run].reshape(VERTICAL_LAYERS, N_DOM, DOMAIN_CAPACITY)
        for outer_step in range(STEPS):
            theta_ext = extend_all(scalar_quantity, export_lists)
            left = at_cells(theta_ext, ends[0])
            right = at_cells(theta_ext, ends[1])
            fluxes = lengths * (0.5 * wind * (left + right) - (0.5 * jnp.abs(wind) + kappa) * (right - left))
            differences = scalar_quantity[1:] - scalar_quantity[:-1]
            zero_row = jnp.zeros((1, N_DOM, DOMAIN_CAPACITY), jnp.float32)
            vertical = mixing * (jnp.concatenate([differences, zero_row], 0) - jnp.concatenate([zero_row, differences], 0))
            advanced = jnp.where(owned, scalar_quantity + time_step * (-inverse * divergence_all(fluxes, incident, edge_sign) + vertical), scalar_quantity)
            forcing = couple * (advanced - scalar_quantity) / NS
            for substep in range(NS):
                press_ext = extend_all(current, export_lists)
                gradient = weights * (at_cells(press_ext, ends[1]) - at_cells(press_ext, ends[0]))
                stepped = jnp.where(owned, 2.0 * current - previous + speed * inverse * divergence_all(gradient, incident, edge_sign) + forcing, current)
                previous, current = current, stepped
            level_mean = (jnp.sum(current * cell_area, axis=(1, 2)) / jnp.sum(cell_area))[:, None, None]
            current = jnp.where(owned, current - level_mean, current)
            previous = jnp.where(owned, previous - level_mean, previous)
            scalar_quantity = advanced
        press_list.append(current.reshape(VERTICAL_LAYERS, CELLS))
        temp_list.append(scalar_quantity.reshape(VERTICAL_LAYERS, CELLS))
    press_all = jnp.stack(press_list)
    temp_all = jnp.stack(temp_list)
    return press_all, temp_all, jnp.sum(press_all, axis=0) / MEMBERS
```

```python
import jax
import jax.numpy as jnp
from jax import lax
from jax.experimental import pallas as pl
from jax.experimental.pallas import tpu as pltpu
from jax.sharding import PartitionSpec as P

MESH = pl.DeviceIdType.MESH
F32 = jnp.float32
BF16 = jnp.bfloat16

LV = 32
CC = 1024
NBK = 6
HB = 128
HALO = NBK * HB
EXT = CC + HALO
LINE = 16
DT = 0.25
NS = 3
OFFSETS = [(b // 2 + 1) * (1 - 2 * (b % 2)) for b in range(NBK)]
GRID = 1024.0


def split2(x):
    hi = x.astype(BF16)
    lo = (x - hi.astype(F32)).astype(BF16)
    return hi, lo


def rows2(x):
    return jnp.concatenate(split2(x), axis=0)


def split3(x):
    a = x.astype(BF16)
    r = x - a.astype(F32)
    b = r.astype(BF16)
    c = (r - b.astype(F32)).astype(BF16)
    return a, b, c


def mm(a, b):
    return jnp.dot(a, b, preferred_element_type=F32)


def mm_t(a, b):
    return lax.dot_general(a, b, (((1,), (1,)), ((), ())), preferred_element_type=F32)


def fold(o):
    return o[:LV] + o[LV : 2 * LV]


def kernel(
    par, tot, p_in, q_in, t_in, v_in, small_in, inv_in, exp_in, end_in,
    p_out, t_out, e_out,
    sel, mat, esel, vd, sd, snd, rcv, row_a, row_b, row_m, box_a, box_b, box_m,
    cur_buf, rs_box, slab, ens, s_send, s_recv, a_send, a_recv, x_send, x_recv,
):
    n_mem = lax.axis_size("member")
    n_dom = lax.axis_size("dom")
    n_line = n_dom // LINE
    m = lax.axis_index("member")
    d = lax.axis_index("dom")
    line, pos = d // LINE, d % LINE

    neighbours = [(m, (d + off + n_dom) % n_dom) for off in OFFSETS]
    in_line = [(m, line * LINE + (pos + k) % LINE) for k in range(1, LINE)]
    across = [(m, (d + k * LINE) % n_dom) for k in range(1, n_line)]
    members = [((m + k) % n_mem, d) for k in range(1, n_mem)]

    barrier = pltpu.get_barrier_semaphore()
    peers = neighbours + in_line + across + members
    for peer in peers:
        pl.semaphore_signal(barrier, inc=1, device_id=peer, device_id_type=MESH)

    speed = par[0, 0]
    kappa = 0.5 * par[0, 1]
    mixing = 0.6 * par[0, 2]
    couple = par[0, 3]
    owned = lax.broadcasted_iota(jnp.int32, (1, CC), 1) < tot[0]
    inv = inv_in[...]
    iota16 = lax.broadcasted_iota(jnp.int32, (16, HB), 0).astype(F32).astype(BF16)
    one = jnp.full((16, HB), 1.0, BF16)
    zero = jnp.full((16, HB), 0.0, BF16)

    def packed_row(row):
        return jnp.broadcast_to(row, (16, HB)).astype(BF16)

    def build_exports(t, carry):
        base = pl.multiple_of(t * 256, 256)
        for b in range(NBK):
            want = exp_in[0, b : b + 1, :].astype(F32) - (t * 256).astype(F32)
            want = packed_row(jnp.clip(want, -1.0, 256.0))
            for r in range(16):
                hit = (iota16 + jnp.asarray(16.0 * r, BF16)) == want
                esel[pl.ds(base + 16 * r, 16), b * HB : (b + 1) * HB] = jnp.where(hit, one, zero)
        return carry

    lax.fori_loop(0, CC // 256, build_exports, 0)

    def store_rows(slot, values):
        for b in range(NBK):
            snd[slot, b] = values[:, b * HB : (b + 1) * HB]

    def halo_copy(slot, b):
        return pltpu.make_async_remote_copy(
            src_ref=snd.at[slot, b],
            dst_ref=rcv.at[slot, b],
            send_sem=s_send.at[slot, b],
            recv_sem=s_recv.at[slot, b],
            device_id=neighbours[b],
            device_id_type=MESH,
        )

    def send(slot):
        for b in range(NBK):
            halo_copy(slot, b).start()

    def receive(slot):
        for b in range(NBK):
            halo_copy(slot, b).wait_recv()
        return jnp.concatenate([rcv[slot, b] for b in range(NBK)], axis=1)

    pres = p_in[0]
    prev = q_in[0]
    theta = t_in[0]
    both = mm(jnp.concatenate([rows2(theta), rows2(pres)], axis=0), esel[...])
    store_rows(6, fold(both[: 2 * LV]))
    store_rows(0, fold(both[2 * LV :]))
    pl.semaphore_wait(barrier, len(peers))
    send(6)
    send(0)

    er = lax.broadcasted_iota(jnp.int32, (3 * HB, 3 * HB), 0)
    ec = lax.broadcasted_iota(jnp.int32, (3 * HB, 3 * HB), 1)
    order = jnp.where(er == 3 * (ec % HB) + ec // HB, 1.0, 0.0).astype(F32).astype(BF16)
    ends = end_in[1:2, :]
    end_hi = (ends // 256).astype(F32)
    end_lo = (ends % 256).astype(F32)
    smalls = jnp.concatenate([end_hi, end_lo, small_in[...], jnp.zeros((4, 3 * CC), F32)], axis=0)
    s1, s2, s3 = split3(smalls)
    v1, v2, v3 = split3(v_in[...])
    stacked = jnp.concatenate([v1, v2, v3], axis=0)
    stacked_small = jnp.concatenate([s1.astype(F32), s2.astype(F32), s3.astype(F32)], axis=0)
    stacked_small = jnp.concatenate([stacked_small, jnp.zeros((8, 3 * CC), F32)], axis=0).astype(BF16)
    for g in range(CC // HB):
        cols = slice(g * 3 * HB, (g + 1) * 3 * HB)
        o = mm(jnp.concatenate([stacked[:, cols], stacked_small[:, cols]], axis=0), order)
        vel = o[:LV] + o[LV : 2 * LV] + o[2 * LV : 3 * LV]
        small = o[96:104] + o[104:112] + o[112:120]
        for j in range(3):
            vd[j, :, g * HB : (g + 1) * HB] = vel[:, j * HB : (j + 1) * HB]
            sd[j, :, g * HB : (g + 1) * HB] = small[:, j * HB : (j + 1) * HB]

    def build(t, carry):
        base = pl.multiple_of(t * 256, 256)
        tf = t.astype(F32)
        for g in range(CC // HB):
            lanes = slice(g * HB, (g + 1) * HB)
            want, whi, wlo = [], [], []
            for j in range(3):
                offset = (sd[j, 0:1, lanes] - tf) * 256.0 + sd[j, 1:2, lanes]
                want.append(packed_row(jnp.clip(offset, -1.0, 256.0)))
                w = sd[j, 3:4, lanes]
                lead = jnp.floor(w * GRID + 0.5) * (1.0 / GRID)
                whi.append(packed_row(lead))
                wlo.append(packed_row(w - lead))
            for r in range(16):
                row = pl.ds(base + 16 * r, 16)
                place = iota16 + jnp.asarray(16.0 * r, BF16)
                hit = [place == want[j] for j in range(3)]
                for j in range(3):
                    sel[j, row, lanes] = jnp.where(hit[j], one, zero)
                hi = [jnp.where(hit[j], whi[j], zero) for j in range(3)]
                lo = [jnp.where(hit[j], wlo[j], zero) for j in range(3)]
                mat[0, row, lanes] = hi[0] + hi[1] + hi[2]
                mat[1, row, lanes] = lo[0] + lo[1] + lo[2]
        return carry

    lax.fori_loop(0, EXT // 256, build, 0)

    def coefficients(j):
        v = vd[j]
        length = sd[j, 2:3, :]
        return length * (jnp.maximum(v, 0.0) + kappa), length * (jnp.minimum(v, 0.0) - kappa)

    def theta_local(th):
        lhs = rows2(th)
        net = jnp.zeros((LV, CC), F32)
        for j in range(3):
            near, far = coefficients(j)
            flux = near * th + far * fold(mm(lhs, sel[j, :CC, :]))
            net = net + flux - fold(mm_t(rows2(flux), sel[j, :CC, :]))
        return net

    def theta_finish(th, net, halo):
        lhs = rows2(halo)
        for j in range(3):
            net = net + coefficients(j)[1] * fold(mm(lhs, sel[j, CC:, :]))
        up = jnp.concatenate([th[1:], th[LV - 1 :]], axis=0) - th
        down = th - jnp.concatenate([th[:1], th[: LV - 1]], axis=0)
        return jnp.where(owned, th + DT * (mixing * (up - down) - inv * net), th)

    ones = jnp.ones((16, CC), BF16)

    def local_rows(p, with_ones=False):
        lhs = rows2(p)
        if with_ones:
            lhs = jnp.concatenate([lhs, ones], axis=0)
        return (
            mm(lhs, mat[0, :CC, :]) + mm(lhs, mat[1, :CC, :])
            + mm_t(lhs, mat[0, :CC, :]) + mm_t(lhs, mat[1, :CC, :])
        )

    def halo_rows(h, with_ones=False):
        lhs = rows2(h)
        if with_ones:
            lhs = jnp.concatenate([lhs, ones[:, :HALO]], axis=0)
        return mm(lhs, mat[0, CC:, :]) + mm(lhs, mat[1, CC:, :])

    scale = speed * inv

    def advance(p, q, near, far, degree, force):
        change = scale * (fold(near) + fold(far) - degree * p) + force
        return jnp.where(owned, 2.0 * p - q + change, p), p

    def export(p):
        return fold(mm(rows2(p), esel[...]))

    area = jnp.where(owned, 1.0 / inv, 0.0)

    def partial_row(p):
        total = jnp.zeros((LV, HB), F32)
        spread = jnp.zeros((1, HB), F32)
        for g in range(CC // HB):
            lanes = slice(g * HB, (g + 1) * HB)
            total = total + p[:, lanes] * area[:, lanes]
            spread = spread + area[:, lanes]
        padded = jnp.concatenate([total, spread, jnp.zeros((HB - LV - 1, HB), F32)], axis=0)
        return jnp.sum(padded.T, axis=0, keepdims=True)

    def spread_row(row):
        return jnp.broadcast_to(row, (HB, HB)).T[:LV]

    def line_copy(which, k):
        return pltpu.make_async_remote_copy(
            src_ref=row_a.at[which],
            dst_ref=box_a.at[which, pos],
            send_sem=a_send.at[which, k],
            recv_sem=a_recv.at[which, k],
            device_id=in_line[k - 1],
            device_id_type=MESH,
        )

    def across_copy(which, k):
        return pltpu.make_async_remote_copy(
            src_ref=row_b.at[which],
            dst_ref=box_b.at[which, line],
            send_sem=a_send.at[which, LINE + k],
            recv_sem=a_recv.at[which, LINE + k],
            device_id=across[k - 1],
            device_id_type=MESH,
        )

    def start_mean(which, p):
        row = partial_row(p)
        row_a[which] = row
        box_a[which, pos] = row
        for k in range(1, LINE):
            line_copy(which, k).start()

    def turn_mean(which):
        for k in range(1, LINE):
            line_copy(which, k).wait_recv()
        row = jnp.sum(box_a[which], axis=0)
        row_b[which] = row
        box_b[which, line] = row
        for k in range(1, n_line):
            across_copy(which, k).start()

    def end_mean(which):
        for k in range(1, n_line):
            across_copy(which, k).wait_recv()
        row = jnp.sum(box_b[which], axis=0)
        return row / row[:, LV : LV + 1]

    def less_mean(p, level_mean):
        wide = jnp.concatenate([level_mean] * (CC // HB), axis=1)
        return p - jnp.where(owned, wide, 0.0)

    net = theta_local(theta)
    near = local_rows(pres, True)
    theta_next = theta_finish(theta, net, receive(6))
    force = couple * (theta_next - theta) / NS
    theta = theta_next
    far = halo_rows(receive(0), True)
    degree = near[2 * LV : 2 * LV + 1] + far[2 * LV : 2 * LV + 1]
    pres, prev = advance(pres, prev, near, far, degree, force)
    store_rows(1, export(pres))
    send(1)
    store_rows(7, export(theta))
    send(7)
    near = local_rows(pres)
    pres, prev = advance(pres, prev, near, halo_rows(receive(1)), degree, force)
    store_rows(2, export(pres))
    send(2)
    near = local_rows(pres)
    net = theta_local(theta)
    pres, prev = advance(pres, prev, near, halo_rows(receive(2)), degree, force)
    store_rows(3, export(pres))
    send(3)
    start_mean(0, pres)
    near = local_rows(pres)
    theta_next = theta_finish(theta, net, receive(7))
    force = couple * (theta_next - theta) / NS
    t_out[0] = theta_next
    pres, prev = advance(pres, prev, near, halo_rows(receive(3)), degree, force)
    store_rows(4, export(pres))
    send(4)
    near = local_rows(pres)
    turn_mean(0)
    pres, prev = advance(pres, prev, near, halo_rows(receive(4)), degree, force)
    store_rows(5, export(pres))
    send(5)
    near = local_rows(pres)
    first_mean = spread_row(end_mean(0))
    pres, prev = advance(pres, prev, near, halo_rows(receive(5)), degree, force)
    current = less_mean(pres, first_mean)
    cur_buf[...] = current

    band = LV // n_mem

    def scatter_copy(k):
        peer = (m + k) % n_mem
        return pltpu.make_async_remote_copy(
            src_ref=cur_buf.at[pl.ds(pl.multiple_of(peer * band, band), band), :],
            dst_ref=rs_box.at[m],
            send_sem=x_send.at[0, k],
            recv_sem=x_recv.at[0, k],
            device_id=members[k - 1],
            device_id_type=MESH,
        )

    def gather_copy(k):
        return pltpu.make_async_remote_copy(
            src_ref=slab,
            dst_ref=ens.at[m],
            send_sem=x_send.at[1, k],
            recv_sem=x_recv.at[1, k],
            device_id=members[k - 1],
            device_id_type=MESH,
        )

    def mean_copy(k):
        return pltpu.make_async_remote_copy(
            src_ref=row_m,
            dst_ref=box_m.at[m],
            send_sem=x_send.at[2, k],
            recv_sem=x_recv.at[2, k],
            device_id=members[k - 1],
            device_id_type=MESH,
        )

    for k in range(1, n_mem):
        scatter_copy(k).start()
    start_mean(1, current)
    rs_box[m] = cur_buf[pl.ds(pl.multiple_of(m * band, band), band), :]
    for k in range(1, n_mem):
        scatter_copy(k).wait_recv()
    total = jnp.sum(rs_box[...], axis=0)
    slab[...] = total
    ens[m] = total
    for k in range(1, n_mem):
        gather_copy(k).start()
    turn_mean(1)
    row = end_mean(1)
    row_m[...] = row
    box_m[m] = row
    for k in range(1, n_mem):
        mean_copy(k).start()
    p_out[0] = less_mean(current, spread_row(row))
    for k in range(1, n_mem):
        gather_copy(k).wait_recv()
    for k in range(1, n_mem):
        mean_copy(k).wait_recv()
    all_means = spread_row(jnp.sum(box_m[...], axis=0))
    summed = jnp.concatenate([ens[i] for i in range(n_mem)], axis=0)
    e_out[...] = less_mean(summed, all_means) / n_mem

    for slot in range(8):
        for b in range(NBK):
            halo_copy(slot, b).wait_send()
    for which in range(2):
        for k in range(1, LINE):
            line_copy(which, k).wait_send()
        for k in range(1, n_line):
            across_copy(which, k).wait_send()
    for k in range(1, n_mem):
        scatter_copy(k).wait_send()
        gather_copy(k).wait_send()
        mean_copy(k).wait_send()


def per_device(
    acoustic_perturbation,
    prior_acoustic_state,
    thermal_anomaly,
    model_parameters,
    crossing_velocity,
    face_extent,
    face_metric_factor,
    reciprocal_polygon_surface,
    owned_totals,
    export_lists,
    face_neighbour_pair,
    polygon_side_lookup,
):
    n_mem = lax.axis_size("member")
    n_line = lax.axis_size("dom") // LINE
    band = LV // n_mem
    smalls = jnp.stack([face_extent, face_metric_factor])
    vmem = pl.BlockSpec(memory_space=pltpu.VMEM)
    smem = pl.BlockSpec(memory_space=pltpu.SMEM)
    dma = pltpu.SemaphoreType.DMA
    return pl.pallas_call(
        kernel,
        out_shape=(
            jax.ShapeDtypeStruct((1, LV, CC), F32),
            jax.ShapeDtypeStruct((1, LV, CC), F32),
            jax.ShapeDtypeStruct((LV, CC), F32),
        ),
        in_specs=[smem, smem] + [vmem] * 8,
        out_specs=(vmem, vmem, vmem),
        scratch_shapes=[
            pltpu.VMEM((3, EXT, CC), BF16),
            pltpu.VMEM((2, EXT, CC), BF16),
            pltpu.VMEM((CC, HALO), BF16),
            pltpu.VMEM((3, LV, CC), F32),
            pltpu.VMEM((3, 8, CC), F32),
            pltpu.VMEM((8, NBK, LV, HB), F32),
            pltpu.VMEM((8, NBK, LV, HB), F32),
            pltpu.VMEM((2, 1, HB), F32),
            pltpu.VMEM((2, 1, HB), F32),
            pltpu.VMEM((1, HB), F32),
            pltpu.VMEM((2, LINE, 1, HB), F32),
            pltpu.VMEM((2, n_line, 1, HB), F32),
            pltpu.VMEM((n_mem, 1, HB), F32),
            pltpu.VMEM((LV, CC), F32),
            pltpu.VMEM((n_mem, band, CC), F32),
            pltpu.VMEM((band, CC), F32),
            pltpu.VMEM((n_mem, band, CC), F32),
            dma((8, NBK)),
            dma((8, NBK)),
            dma((2, LINE + n_line)),
            dma((2, LINE + n_line)),
            dma((3, n_mem)),
            dma((3, n_mem)),
        ],
        compiler_params=pltpu.CompilerParams(collective_id=0, has_side_effects=True),
    )(
        model_parameters,
        owned_totals,
        acoustic_perturbation,
        prior_acoustic_state,
        thermal_anomaly,
        crossing_velocity,
        smalls,
        reciprocal_polygon_surface[None, :],
        export_lists,
        face_neighbour_pair,
    )


def solution(mesh):
    in_specs = (
        P("member", None, "dom"),
        P("member", None, "dom"),
        P("member", None, "dom"),
        P("member", None),
        P(None, "dom"),
        P("dom"),
        P("dom"),
        P("dom"),
        P("dom"),
        P("dom", None, None),
        P(None, "dom"),
        P(None, "dom"),
    )
    out_specs = (P("member", None, "dom"), P("member", None, "dom"), P(None, "dom"))
    return jax.shard_map(
        per_device, mesh=mesh, in_specs=in_specs, out_specs=out_specs, check_vma=False
    )
```

```python
import jax
import jax.numpy as jnp
from jax import lax
from jax.experimental import pallas as pl
from jax.experimental.pallas import tpu as pltpu
from jax.sharding import PartitionSpec as P

MESH = pl.DeviceIdType.MESH
F32 = jnp.float32
BF16 = jnp.bfloat16
F8 = jnp.float8_e4m3fn

LV = 32
CC = 1024
NBK = 6
HB = 128
HALO = NBK * HB
EXT = CC + HALO
LINE = 16
DT = 0.25
NS = 3
OFFSETS = [(b // 2 + 1) * (1 - 2 * (b % 2)) for b in range(NBK)]
SEND_ORDER = (4, 5, 2, 3, 0, 1)


def split2(x):
    hi = x.astype(BF16)
    lo = (x - hi.astype(F32)).astype(BF16)
    return hi, lo


def rows2(*fields):
    return jnp.concatenate([part for x in fields for part in split2(x)], axis=0)


def split3(x):
    a = x.astype(BF16)
    r = x - a.astype(F32)
    b = r.astype(BF16)
    c = (r - b.astype(F32)).astype(BF16)
    return a, b, c


def mm(a, b):
    return jnp.dot(a, b, preferred_element_type=F32)


def mm_t(a, b):
    return lax.dot_general(a, b, (((1,), (1,)), ((), ())), preferred_element_type=F32)


def fold(o, i=0):
    return o[2 * i * LV : (2 * i + 1) * LV] + o[(2 * i + 1) * LV : (2 * i + 2) * LV]


def kernel(
    par, tot, p_hbm, q_hbm, t_hbm, v_hbm, len_in, met_in, inv_in, exp_in, end_in,
    p_out, t_out, e_out,
    p_in, q_in, t_in, v_in, sel, esel, vd, sd, snd, rcv, row_a, row_b, box_a, box_b, box_x,
    cur_buf, rs_box, slab, ens, in_sem, s_send, s_recv, a_send, a_recv, b_send, b_recv, x_send, x_recv,
):
    n_mem = lax.axis_size("member")
    n_dom = lax.axis_size("dom")
    n_line = n_dom // LINE
    m = lax.axis_index("member")
    d = lax.axis_index("dom")
    line, pos = d // LINE, d % LINE

    loads = [
        pltpu.make_async_copy(src, dst, in_sem.at[i])
        for i, (src, dst) in enumerate(((t_hbm.at[0], t_in), (p_hbm.at[0], p_in), (v_hbm, v_in), (q_hbm.at[0], q_in)))
    ]
    for load in loads:
        load.start()

    neighbours = [(m, (d + off + n_dom) % n_dom) for off in OFFSETS]
    in_line = [(m, line * LINE + (pos + k) % LINE) for k in range(1, LINE)]
    shifts = [(i, k) for i in range(n_mem) for k in range(n_line) if i or k]
    across = [((m + i) % n_mem, (d + k * LINE) % n_dom) for i, k in shifts]
    members = [((m + k) % n_mem, d) for k in range(1, n_mem)]

    barrier = pltpu.get_barrier_semaphore()
    peers = neighbours + in_line + across
    for peer in peers:
        pl.semaphore_signal(barrier, inc=1, device_id=peer, device_id_type=MESH)

    speed = par[0, 0]
    kappa = 0.5 * par[0, 1]
    mixing = 0.6 * par[0, 2]
    couple = par[0, 3]
    owned = lax.broadcasted_iota(jnp.int32, (1, CC), 1) < tot[0]
    inv = inv_in[...]
    iota32 = lax.broadcasted_iota(jnp.int32, (32, HB), 0).astype(F32).astype(BF16)
    one = jnp.full((32, HB), 1.0, BF16)
    zero = jnp.full((32, HB), 0.0, BF16)

    def packed_row(row):
        return jnp.broadcast_to(jnp.clip(row, -1.0, 256.0), (32, HB)).astype(BF16)

    def hot(r, want):
        return jnp.where(iota32 + jnp.asarray(32.0 * r, BF16) == want, one, zero).astype(F8)

    def build_exports(t, carry):
        base = pl.multiple_of(t * 256, 256)
        for b in range(NBK):
            want = packed_row(exp_in[b].astype(F32) - (t * 256).astype(F32))
            for r in range(8):
                esel[pl.ds(base + 32 * r, 32), b * HB : (b + 1) * HB] = hot(r, want)
        return carry

    lax.fori_loop(0, CC // 256, build_exports, 0)

    def store_rows(slot, values):
        for b in range(NBK):
            snd[slot, b] = values[:, b * HB : (b + 1) * HB]

    def halo_copy(slot, b):
        return pltpu.make_async_remote_copy(
            src_ref=snd.at[slot, b],
            dst_ref=rcv.at[slot, b],
            send_sem=s_send.at[slot, b],
            recv_sem=s_recv.at[slot, b],
            device_id=neighbours[b],
            device_id_type=MESH,
        )

    def send(slot):
        for b in SEND_ORDER:
            halo_copy(slot, b).start()

    def receive(slot):
        for b in range(NBK):
            halo_copy(slot, b).wait_recv()
        return jnp.concatenate([rcv[slot, b] for b in range(NBK)], axis=1)

    loads[0].wait()
    loads[1].wait()
    theta = t_in[...]
    pres = p_in[...]
    both = mm(rows2(theta, pres), esel[...])
    store_rows(6, fold(both, 0))
    store_rows(0, fold(both, 1))

    er = lax.broadcasted_iota(jnp.int32, (3 * HB, 3 * HB), 0)
    ec = lax.broadcasted_iota(jnp.int32, (3 * HB, 3 * HB), 1)
    order = jnp.where(er == 3 * (ec % HB) + ec // HB, 1.0, 0.0).astype(F32).astype(BF16)
    ends = end_in[1:2, :]
    end_hi = (ends // 256).astype(F32)
    end_lo = (ends % 256).astype(F32)
    smalls = jnp.concatenate([end_hi, end_lo, len_in[...], met_in[...], jnp.zeros((4, 3 * CC), F32)], axis=0)
    smalls = jnp.concatenate(
        [part.astype(F32) for part in split3(smalls)] + [jnp.zeros((8, 3 * CC), F32)], axis=0
    ).astype(BF16)
    loads[2].wait()
    stacked = rows2(v_in[...])
    for g in range(CC // HB):
        cols = slice(g * 3 * HB, (g + 1) * 3 * HB)
        o = mm(jnp.concatenate([stacked[:, cols], smalls[:, cols]], axis=0), order)
        vel = fold(o)
        small = o[64:72] + o[72:80] + o[80:88]
        for j in range(3):
            vd[j, :, g * HB : (g + 1) * HB] = vel[:, j * HB : (j + 1) * HB]
            sd[j, :, g * HB : (g + 1) * HB] = small[:, j * HB : (j + 1) * HB]

    def build(t, carry):
        base = pl.multiple_of(t * 256, 256)
        tf = t.astype(F32)
        for g in range(CC // HB):
            lanes = slice(g * HB, (g + 1) * HB)
            for j in range(3):
                want = packed_row((sd[j, 0:1, lanes] - tf) * 256.0 + sd[j, 1:2, lanes])
                for r in range(8):
                    sel[j, pl.ds(base + 32 * r, 32), lanes] = hot(r, want)
        return carry

    lax.fori_loop(0, CC // 256, build, 0)
    pl.semaphore_wait(barrier, len(peers))
    send(6)
    send(0)
    lax.fori_loop(CC // 256, EXT // 256, build, 0)

    def coefficients(j):
        v = vd[j]
        length = sd[j, 2:3, :]
        return length * (jnp.maximum(v, 0.0) + kappa), length * (jnp.minimum(v, 0.0) - kappa)

    def weight(j):
        return sd[j, 3:4, :]

    def near_both(p, th):
        lhs = rows2(p, th)
        net_p, net_t = jnp.zeros((LV, CC), F32), jnp.zeros((LV, CC), F32)
        for j in range(3):
            ends_of = mm(lhs, sel[j, :CC, :])
            start, end = coefficients(j)
            grad = weight(j) * (fold(ends_of, 0) - p)
            flux = start * th + end * fold(ends_of, 1)
            incoming = mm_t(rows2(grad, flux), sel[j, :CC, :])
            net_p = net_p + grad - fold(incoming, 0)
            net_t = net_t + flux - fold(incoming, 1)
        return net_p, net_t

    def near_pressure(p):
        lhs = rows2(p)
        net = jnp.zeros((LV, CC), F32)
        for j in range(3):
            grad = weight(j) * (fold(mm(lhs, sel[j, :CC, :])) - p)
            net = net + grad - fold(mm_t(rows2(grad), sel[j, :CC, :]))
        return net

    def far_pressure(halo, net):
        lhs = rows2(halo)
        for j in range(3):
            net = net + weight(j) * fold(mm(lhs, sel[j, CC:, :]))
        return net

    def far_theta(halo, net):
        lhs = rows2(halo)
        for j in range(3):
            net = net + coefficients(j)[1] * fold(mm(lhs, sel[j, CC:, :]))
        return net

    def advance_theta(th, net):
        up = jnp.concatenate([th[1:], th[LV - 1 :]], axis=0) - th
        down = th - jnp.concatenate([th[:1], th[: LV - 1]], axis=0)
        return jnp.where(owned, th + DT * (mixing * (up - down) - inv * net), th)

    scale = speed * inv

    def advance(p, q, net, force):
        return jnp.where(owned, 2.0 * p - q + scale * net + force, p), p

    def export(p):
        return fold(mm(rows2(p), esel[...]))

    area = jnp.where(owned, 1.0 / inv, 0.0)

    def partial_row(p):
        total = jnp.zeros((LV, HB), F32)
        spread = jnp.zeros((1, HB), F32)
        for g in range(CC // HB):
            lanes = slice(g * HB, (g + 1) * HB)
            total = total + p[:, lanes] * area[:, lanes]
            spread = spread + area[:, lanes]
        padded = jnp.concatenate([total, spread, jnp.zeros((HB - LV - 1, HB), F32)], axis=0)
        return jnp.sum(padded.T, axis=0, keepdims=True)

    def spread_row(row):
        return jnp.broadcast_to(row, (HB, HB)).T[:LV]

    def line_copy(which, k):
        return pltpu.make_async_remote_copy(
            src_ref=row_a.at[which],
            dst_ref=box_a.at[which, pos],
            send_sem=a_send.at[which, k],
            recv_sem=a_recv.at[which, k],
            device_id=in_line[k - 1],
            device_id_type=MESH,
        )

    def across_copy(k):
        return pltpu.make_async_remote_copy(
            src_ref=row_b.at[0],
            dst_ref=box_b.at[line],
            send_sem=b_send.at[0, k],
            recv_sem=b_recv.at[0, k],
            device_id=(m, (d + k * LINE) % n_dom),
            device_id_type=MESH,
        )

    def wide_copy(n):
        return pltpu.make_async_remote_copy(
            src_ref=row_b.at[1],
            dst_ref=box_x.at[m, line],
            send_sem=b_send.at[1, n],
            recv_sem=b_recv.at[1, n],
            device_id=across[n],
            device_id_type=MESH,
        )

    def start_mean(which, p):
        row = partial_row(p)
        row_a[which] = row
        box_a[which, pos] = row
        for k in range(1, LINE):
            line_copy(which, k).start()

    def line_sum(which):
        for k in range(1, LINE):
            line_copy(which, k).wait_recv()
        row = jnp.sum(box_a[which], axis=0)
        row_b[which] = row
        return row

    def level_mean(rows):
        row = jnp.sum(rows, axis=0)
        return row / row[:, LV : LV + 1]

    def less_mean(p, mean):
        wide = jnp.concatenate([spread_row(mean)] * (CC // HB), axis=1)
        return p - jnp.where(owned, wide, 0.0)

    net, net_theta = near_both(pres, theta)
    theta_next = advance_theta(theta, far_theta(receive(6), net_theta))
    force = couple * (theta_next - theta) / NS
    theta = theta_next
    net = far_pressure(receive(0), net)
    loads[3].wait()
    pres, prev = advance(pres, q_in[...], net, force)
    store_rows(1, export(pres))
    send(1)
    store_rows(7, export(theta))
    send(7)
    net = near_pressure(pres)
    pres, prev = advance(pres, prev, far_pressure(receive(1), net), force)
    store_rows(2, export(pres))
    send(2)
    net, net_theta = near_both(pres, theta)
    pres, prev = advance(pres, prev, far_pressure(receive(2), net), force)
    store_rows(3, export(pres))
    send(3)
    start_mean(0, pres)
    net = near_pressure(pres)
    theta_next = advance_theta(theta, far_theta(receive(7), net_theta))
    force = couple * (theta_next - theta) / NS
    t_out[...] = theta_next
    pres, prev = advance(pres, prev, far_pressure(receive(3), net), force)
    store_rows(4, export(pres))
    send(4)
    net = near_pressure(pres)
    row = line_sum(0)
    box_b[line] = row
    for k in range(1, n_line):
        across_copy(k).start()
    pres, prev = advance(pres, prev, far_pressure(receive(4), net), force)
    store_rows(5, export(pres))
    send(5)
    net = near_pressure(pres)
    for k in range(1, n_line):
        across_copy(k).wait_recv()
    first_mean = level_mean(box_b[...])
    pres, prev = advance(pres, prev, far_pressure(receive(5), net), force)
    current = less_mean(pres, first_mean)
    cur_buf[...] = current

    band = LV // n_mem

    def scatter_copy(k):
        peer = (m + k) % n_mem
        return pltpu.make_async_remote_copy(
            src_ref=cur_buf.at[pl.ds(pl.multiple_of(peer * band, band), band), :],
            dst_ref=rs_box.at[m],
            send_sem=x_send.at[0, k],
            recv_sem=x_recv.at[0, k],
            device_id=members[k - 1],
            device_id_type=MESH,
        )

    def gather_copy(k):
        return pltpu.make_async_remote_copy(
            src_ref=slab,
            dst_ref=ens.at[m],
            send_sem=x_send.at[1, k],
            recv_sem=x_recv.at[1, k],
            device_id=members[k - 1],
            device_id_type=MESH,
        )

    for k in range(1, n_mem):
        scatter_copy(k).start()
    start_mean(1, current)
    rs_box[m] = cur_buf[pl.ds(pl.multiple_of(m * band, band), band), :]
    for k in range(1, n_mem):
        scatter_copy(k).wait_recv()
    total = jnp.sum(rs_box[...], axis=0)
    slab[...] = total
    ens[m] = total
    for k in range(1, n_mem):
        gather_copy(k).start()
    row = line_sum(1)
    box_x[m, line] = row
    for n in range(len(shifts)):
        wide_copy(n).start()
    for k in range(1, n_mem):
        gather_copy(k).wait_recv()
    for n in range(len(shifts)):
        wide_copy(n).wait_recv()
    p_out[...] = less_mean(current, level_mean(box_x[m]))
    all_means = level_mean(box_x[0])
    for i in range(1, n_mem):
        all_means = all_means + level_mean(box_x[i])
    summed = jnp.concatenate([ens[i] for i in range(n_mem)], axis=0)
    e_out[...] = less_mean(summed, all_means) / n_mem

    for slot in range(8):
        for b in range(NBK):
            halo_copy(slot, b).wait_send()
    for which in range(2):
        for k in range(1, LINE):
            line_copy(which, k).wait_send()
    for k in range(1, n_line):
        across_copy(k).wait_send()
    for n in range(len(shifts)):
        wide_copy(n).wait_send()
    for k in range(1, n_mem):
        scatter_copy(k).wait_send()
        gather_copy(k).wait_send()


def hand_over(p, t, e, p_out, t_out, e_out, sem):
    moves = [
        pltpu.make_async_copy(src, dst, sem.at[i])
        for i, (src, dst) in enumerate(((p, p_out.at[0]), (t, t_out.at[0]), (e, e_out)))
    ]
    for move in moves:
        move.start()
    for move in moves:
        move.wait()


def per_device(
    acoustic_perturbation,
    prior_acoustic_state,
    thermal_anomaly,
    model_parameters,
    crossing_velocity,
    face_extent,
    face_metric_factor,
    reciprocal_polygon_surface,
    owned_totals,
    export_lists,
    face_neighbour_pair,
    polygon_side_lookup,
):
    n_mem = lax.axis_size("member")
    n_line = lax.axis_size("dom") // LINE
    n_wide = n_mem * n_line - 1
    band = LV // n_mem
    vmem = pl.BlockSpec(memory_space=pltpu.VMEM)
    smem = pl.BlockSpec(memory_space=pltpu.SMEM)
    anyw = pl.BlockSpec(memory_space=pl.ANY)
    dma = pltpu.SemaphoreType.DMA
    held = pl.pallas_call(
        kernel,
        out_shape=tuple(pltpu.VMEM((LV, CC), F32) for _ in range(3)),
        in_specs=[smem, smem] + [anyw] * 4 + [vmem] * 5,
        out_specs=(vmem, vmem, vmem),
        scratch_shapes=[
            pltpu.VMEM((LV, CC), F32),
            pltpu.VMEM((LV, CC), F32),
            pltpu.VMEM((LV, CC), F32),
            pltpu.VMEM((LV, 3 * CC), F32),
            pltpu.VMEM((3, EXT, CC), F8),
            pltpu.VMEM((CC, HALO), F8),
            pltpu.VMEM((3, LV, CC), F32),
            pltpu.VMEM((3, 8, CC), F32),
            pltpu.VMEM((8, NBK, LV, HB), F32),
            pltpu.VMEM((8, NBK, LV, HB), F32),
            pltpu.VMEM((2, 1, HB), F32),
            pltpu.VMEM((2, 1, HB), F32),
            pltpu.VMEM((2, LINE, 1, HB), F32),
            pltpu.VMEM((n_line, 1, HB), F32),
            pltpu.VMEM((n_mem, n_line, 1, HB), F32),
            pltpu.VMEM((LV, CC), F32),
            pltpu.VMEM((n_mem, band, CC), F32),
            pltpu.VMEM((band, CC), F32),
            pltpu.VMEM((n_mem, band, CC), F32),
            dma((4,)),
            dma((8, NBK)),
            dma((8, NBK)),
            dma((2, LINE)),
            dma((2, LINE)),
            dma((2, n_wide)),
            dma((2, n_wide)),
            dma((2, n_mem)),
            dma((2, n_mem)),
        ],
        compiler_params=pltpu.CompilerParams(collective_id=0, has_side_effects=True),
    )(
        model_parameters,
        owned_totals,
        acoustic_perturbation,
        prior_acoustic_state,
        thermal_anomaly,
        crossing_velocity,
        face_extent[None, :],
        face_metric_factor[None, :],
        reciprocal_polygon_surface[None, :],
        export_lists.reshape(NBK, 1, HB),
        face_neighbour_pair,
    )
    return pl.pallas_call(
        hand_over,
        out_shape=(
            jax.ShapeDtypeStruct((1, LV, CC), F32),
            jax.ShapeDtypeStruct((1, LV, CC), F32),
            jax.ShapeDtypeStruct((LV, CC), F32),
        ),
        in_specs=[vmem] * 3,
        out_specs=(anyw, anyw, anyw),
        scratch_shapes=[dma((3,))],
    )(*[pltpu.with_memory_space_constraint(x, pltpu.VMEM) for x in held])


def solution(mesh):
    in_specs = (
        P("member", None, "dom"),
        P("member", None, "dom"),
        P("member", None, "dom"),
        P("member", None),
        P(None, "dom"),
        P("dom"),
        P("dom"),
        P("dom"),
        P("dom"),
        P("dom", None, None),
        P(None, "dom"),
        P(None, "dom"),
    )
    out_specs = (P("member", None, "dom"), P("member", None, "dom"), P(None, "dom"))
    return jax.shard_map(
        per_device, mesh=mesh, in_specs=in_specs, out_specs=out_specs, check_vma=False
    )
```

```python
import jax
import jax.numpy as jnp
from jax import lax
from jax.experimental import pallas as pl
from jax.experimental.pallas import tpu as pltpu
from jax.sharding import PartitionSpec as P

MESH = pl.DeviceIdType.MESH
F32 = jnp.float32
BF16 = jnp.bfloat16
F8 = jnp.float8_e4m3fn

LV = 32
CC = 1024
NBK = 6
HB = 128
HALO = NBK * HB
EXT = CC + HALO
LINE = 16
DT = 0.25
NS = 3
OFFSETS = [(b // 2 + 1) * (1 - 2 * (b % 2)) for b in range(NBK)]
SEND_ORDER = (4, 5, 2, 3, 0, 1)
NEAR = 4


def split2(x):
    hi = x.astype(BF16)
    lo = (x - hi.astype(F32)).astype(BF16)
    return hi, lo


def rows2(*fields):
    return jnp.concatenate([part for x in fields for part in split2(x)], axis=0)


def split3(x):
    a = x.astype(BF16)
    r = x - a.astype(F32)
    b = r.astype(BF16)
    c = (r - b.astype(F32)).astype(BF16)
    return a, b, c


def mm(a, b):
    return jnp.dot(a, b, preferred_element_type=F32)


def mm_t(a, b):
    return lax.dot_general(a, b, (((1,), (1,)), ((), ())), preferred_element_type=F32)


def fold(o, i=0):
    return o[2 * i * LV : (2 * i + 1) * LV] + o[(2 * i + 1) * LV : (2 * i + 2) * LV]


def kernel(
    par_hbm, p_hbm, q_hbm, t_hbm, v_hbm, len_hbm, met_hbm, inv_hbm, exp_hbm, end_hbm,
    p_out, t_out, e_out,
    par, p_in, q_in, t_in, v_in, len_in, met_in, inv_in, exp_in, end_in,
    sel, esel, vd, sd, snd, rcv, reach, reach_in, row_a, row_b, box_a, box_x, cur_buf, rs_box, slab, ens,
    in_sem, s_send, s_recv, h_sem, a_send, a_recv, b_send, b_recv, x_send, x_recv,
):
    n_mem = lax.axis_size("member")
    n_dom = lax.axis_size("dom")
    n_line = n_dom // LINE
    m = lax.axis_index("member")
    d = lax.axis_index("dom")
    line, pos = d // LINE, d % LINE

    neighbours = [(m, (d + off + n_dom) % n_dom) for off in OFFSETS]
    in_line = [(m, line * LINE + (pos + k) % LINE) for k in range(1, LINE)]
    shifts = [(i, k) for i in range(n_mem) for k in range(n_line) if i or k]
    across = [((m + i) % n_mem, (d + k * LINE) % n_dom) for i, k in shifts]

    barrier = pltpu.get_barrier_semaphore()
    peers = neighbours + in_line + across
    for peer in peers:
        pl.semaphore_signal(barrier, inc=1, device_id=peer, device_id_type=MESH)

    sources = (exp_hbm, t_hbm.at[0], p_hbm.at[0], end_hbm, len_hbm, met_hbm, v_hbm, inv_hbm, par_hbm, q_hbm.at[0])
    targets = (exp_in, t_in, p_in, end_in, len_in, met_in, v_in, inv_in, par, q_in)
    groups = (0, 1, 1, 2, 2, 2, 3, 3, 3, 3)
    loads = [
        pltpu.make_async_copy(src, dst, in_sem.at[i]) for i, (src, dst) in enumerate(zip(sources, targets))
    ]
    for load in loads:
        load.start()

    def loaded(group):
        for load, its in zip(loads, groups):
            if its == group:
                load.wait()

    iota32 = lax.broadcasted_iota(jnp.int32, (32, HB), 0).astype(F32).astype(BF16)
    one = jnp.full((32, HB), 1.0, BF16)
    zero = jnp.full((32, HB), 0.0, BF16)

    def packed_row(row):
        return jnp.broadcast_to(jnp.clip(row, -1.0, 256.0), (32, HB)).astype(BF16)

    def hot(r, want):
        return jnp.where(iota32 + jnp.asarray(32.0 * r, BF16) == want, one, zero).astype(F8)

    loaded(0)

    def build_exports(t, carry):
        base = pl.multiple_of(t * 256, 256)
        for b in range(NBK):
            want = packed_row(exp_in[b].astype(F32) - (t * 256).astype(F32))
            for r in range(8):
                esel[pl.ds(base + 32 * r, 32), b * HB : (b + 1) * HB] = hot(r, want)
        return carry

    lax.fori_loop(0, CC // 256, build_exports, 0)

    def halo_copy(slot, b):
        return pltpu.make_async_remote_copy(
            src_ref=snd.at[slot, b],
            dst_ref=rcv.at[slot, b],
            send_sem=s_send,
            recv_sem=s_recv.at[slot, b // NEAR],
            device_id=neighbours[b],
            device_id_type=MESH,
        )

    def export_and_send(*slots_and_fields):
        slots, fields = slots_and_fields[::2], slots_and_fields[1::2]
        lhs = rows2(*fields)
        for blocks in (range(NEAR, NBK), range(NEAR)):
            o = mm(lhs, esel[:, blocks[0] * HB : (blocks[-1] + 1) * HB])
            for i, slot in enumerate(slots):
                values = fold(o, i)
                for b in blocks:
                    snd[slot, b] = values[:, (b - blocks[0]) * HB : (b - blocks[0] + 1) * HB]
            if slots[0] == 6:
                if blocks[0] == NEAR:
                    continue
                pl.semaphore_wait(barrier, len(peers))
                blocks = SEND_ORDER
            for slot in slots:
                for b in blocks:
                    halo_copy(slot, b).start()

    def arrived(slot, far):
        part = rcv.at[slot, pl.ds(NEAR, NBK - NEAR)] if far else rcv.at[slot, pl.ds(0, NEAR)]
        pltpu.make_async_copy(part, part, s_recv.at[slot, int(far)]).wait()
        blocks = range(NEAR, NBK) if far else range(NEAR)
        return rows2(jnp.concatenate([rcv[slot, b] for b in blocks], axis=1))

    loaded(1)
    theta = t_in[...]
    pres = p_in[...]
    export_and_send(6, theta, 0, pres)

    er = lax.broadcasted_iota(jnp.int32, (3 * HB, 3 * HB), 0)
    ec = lax.broadcasted_iota(jnp.int32, (3 * HB, 3 * HB), 1)
    order = jnp.where(er == 3 * (ec % HB) + ec // HB, 1.0, 0.0).astype(F32).astype(BF16).astype(F8)
    loaded(2)
    ends = end_in[1:2, :]
    smalls = [(ends // 256).astype(F32), (ends % 256).astype(F32)]
    smalls += [part.astype(F32) for row in (len_in, met_in) for part in split3(row[...])]
    smalls = jnp.concatenate(smalls + [jnp.zeros((8, 3 * CC), F32)], axis=0).astype(BF16)
    loaded(3)
    speed = par[0, 0]
    kappa = 0.5 * par[0, 1]
    mixing = 0.6 * par[0, 2]
    couple = par[0, 3]
    inv = inv_in[...]
    stacked = jnp.concatenate([rows2(v_in[...]), smalls], axis=0)
    for g in range(CC // HB):
        o = mm(stacked[:, g * 3 * HB : (g + 1) * 3 * HB], order)
        vel = fold(o)
        small = jnp.concatenate(
            [o[64:65], o[65:66], o[66:67] + o[67:68] + o[68:69], o[69:70] + o[70:71] + o[71:72], o[76:80]], axis=0
        )
        for j in range(3):
            vd[j, :, g * HB : (g + 1) * HB] = vel[:, j * HB : (j + 1) * HB]
            sd[j, :, g * HB : (g + 1) * HB] = small[:, j * HB : (j + 1) * HB]

    owned = sd[0, 0:1, :] < EXT // 256

    def build(t, carry):
        base = pl.multiple_of(t * 256, 256)
        tf = t.astype(F32)
        for g in range(CC // HB):
            lanes = slice(g * HB, (g + 1) * HB)
            for j in range(3):
                want = packed_row((sd[j, 0:1, lanes] - tf) * 256.0 + sd[j, 1:2, lanes])
                for r in range(8):
                    sel[j, pl.ds(base + 32 * r, 32), lanes] = hot(r, want)
        return carry

    lax.fori_loop(0, EXT // 256, build, 0)

    def coefficients(j):
        v = vd[j]
        length = sd[j, 2:3, :]
        return length * (jnp.maximum(v, 0.0) + kappa), length * (jnp.minimum(v, 0.0) - kappa)

    def weight(j):
        return sd[j, 3:4, :]

    def near_both(p, th):
        lhs = rows2(p, th)
        net_p, net_t = jnp.zeros((LV, CC), F32), jnp.zeros((LV, CC), F32)
        for j in range(3):
            ends_of = mm(lhs, sel[j, :CC, :])
            start, end = coefficients(j)
            grad = weight(j) * (fold(ends_of, 0) - p)
            flux = start * th + end * fold(ends_of, 1)
            incoming = mm_t(rows2(grad, flux), sel[j, :CC, :])
            net_p = net_p + grad - fold(incoming, 0)
            net_t = net_t + flux - fold(incoming, 1)
        return net_p, net_t

    def near_pressure(p):
        lhs = rows2(p)
        net = jnp.zeros((LV, CC), F32)
        for j in range(3):
            grad = weight(j) * (fold(mm(lhs, sel[j, :CC, :])) - p)
            net = net + grad - fold(mm_t(rows2(grad), sel[j, :CC, :]))
        return net

    def far_part(slot, scales, net):
        split = CC + NEAR * HB
        lhs = arrived(slot, False)
        for j in range(3):
            net = net + scales[j] * fold(mm(lhs, sel[j, CC:split, :]))
        lhs = arrived(slot, True)
        for j in range(3):
            net = net + scales[j] * fold(mm(lhs, sel[j, split:, :]))
        return net

    def far_pressure(slot, net):
        return far_part(slot, [weight(j) for j in range(3)], net)

    def far_theta(slot, net):
        return far_part(slot, [coefficients(j)[1] for j in range(3)], net)

    def advance_theta(th, net):
        up = jnp.concatenate([th[1:], th[LV - 1 :]], axis=0) - th
        down = th - jnp.concatenate([th[:1], th[: LV - 1]], axis=0)
        return jnp.where(owned, th + DT * (mixing * (up - down) - inv * net), th)

    scale = speed * inv

    def advance(p, q, net, force):
        return jnp.where(owned, 2.0 * p - q + scale * net + force, p), p

    area = jnp.where(owned, 1.0 / inv, 0.0)

    def by_lane(p, factor):
        return sum(
            p[:, g * HB : (g + 1) * HB] * factor[:, g * HB : (g + 1) * HB] for g in range(CC // HB)
        )

    def partial_row(total):
        spread = by_lane(jnp.ones((1, CC), F32), area)
        padded = jnp.concatenate([total, spread, jnp.zeros((HB - LV - 1, HB), F32)], axis=0)
        return jnp.sum(padded.T, axis=0, keepdims=True)

    def reach_copy(b):
        return pltpu.make_async_remote_copy(
            src_ref=reach.at[b],
            dst_ref=reach_in.at[b],
            send_sem=h_sem.at[0],
            recv_sem=h_sem.at[1],
            device_id=(m, (d - OFFSETS[b] + n_dom) % n_dom),
            device_id_type=MESH,
        )

    def send_reach():
        total = jnp.zeros((16, HALO), F32)
        for j in range(3):
            parts = jnp.concatenate([part.astype(F32) for part in split3(weight(j))] + [jnp.zeros((13, CC), F32)], axis=0)
            total = total + mm_t(parts.astype(BF16), sel[j, CC:, :])
        total = jnp.sum(total, axis=0, keepdims=True)
        for b in range(NBK):
            reach[b] = total[:, b * HB : (b + 1) * HB]
            reach_copy(b).start()

    def next_total(slot, p, q, force):
        pltpu.make_async_copy(reach_in, reach_in, h_sem.at[1]).wait()
        leaving = jnp.zeros((1, CC), F32)
        for j in range(3):
            block = sd[j, 0:1, :]
            leaving = leaving + jnp.where((block >= CC // 256) & (block < EXT // 256), weight(j), 0.0)
        total = by_lane(2.0 * p - q + force, area) - speed * by_lane(p, leaving)
        for b in range(NBK):
            total = total + speed * (snd[slot, b] * reach_in[b])
        return total

    def spread_row(row):
        return jnp.broadcast_to(row, (HB, HB)).T[:LV]

    def line_copy(which, k):
        return pltpu.make_async_remote_copy(
            src_ref=row_a.at[which],
            dst_ref=box_a.at[which, pos],
            send_sem=a_send,
            recv_sem=a_recv.at[which],
            device_id=in_line[k],
            device_id_type=MESH,
        )

    def wide_copy(which, n):
        return pltpu.make_async_remote_copy(
            src_ref=row_b.at[which],
            dst_ref=box_x.at[which, m * n_line + line],
            send_sem=b_send,
            recv_sem=b_recv.at[which],
            device_id=across[n],
            device_id_type=MESH,
        )

    def start_mean(which, total):
        row = partial_row(total)
        row_a[which] = row
        for k in range(LINE - 1):
            line_copy(which, k).start()
        box_a[which, pos] = row

    def turn_mean(which):
        others = box_a.at[which, pl.ds(0, LINE - 1)]
        pltpu.make_async_copy(others, others, a_recv.at[which]).wait()
        row = jnp.sum(box_a[which], axis=0)
        row_b[which] = row
        for n in range(len(shifts)):
            wide_copy(which, n).start()
        box_x[which, m * n_line + line] = row

    def end_mean(which):
        others = box_x.at[which, pl.ds(0, len(shifts))]
        pltpu.make_async_copy(others, others, b_recv.at[which]).wait()

    def mean_of(which, member):
        return level_mean(box_x[which, pl.ds(member * n_line, n_line)])

    def level_mean(rows):
        row = jnp.sum(rows, axis=0)
        return row / row[:, LV : LV + 1]

    def less_mean(p, mean):
        wide = jnp.concatenate([spread_row(mean)] * (CC // HB), axis=1)
        return p - jnp.where(owned, wide, 0.0)

    net, net_theta = near_both(pres, theta)
    theta_next = advance_theta(theta, far_theta(6, net_theta))
    force = couple * (theta_next - theta) / NS
    theta = theta_next
    pres, prev = advance(pres, q_in[...], far_pressure(0, net), force)
    export_and_send(1, pres)
    export_and_send(7, theta)
    net = near_pressure(pres)
    send_reach()
    pres, prev = advance(pres, prev, far_pressure(1, net), force)
    export_and_send(2, pres)
    net, net_theta = near_both(pres, theta)
    pres, prev = advance(pres, prev, far_pressure(2, net), force)
    export_and_send(3, pres)
    start_mean(0, by_lane(pres, area))
    net = near_pressure(pres)
    theta_next = advance_theta(theta, far_theta(7, net_theta))
    force = couple * (theta_next - theta) / NS
    t_out[...] = theta_next
    pres, prev = advance(pres, prev, far_pressure(3, net), force)
    export_and_send(4, pres)
    net = near_pressure(pres)
    turn_mean(0)
    pres, prev = advance(pres, prev, far_pressure(4, net), force)
    export_and_send(5, pres)
    start_mean(1, next_total(5, pres, prev, force))
    net = near_pressure(pres)
    end_mean(0)
    pres, prev = advance(pres, prev, far_pressure(5, net), force)
    current = less_mean(pres, mean_of(0, m))
    cur_buf[...] = current

    band = LV // n_mem

    def scatter_copy(k):
        peer = (m + k) % n_mem
        return pltpu.make_async_remote_copy(
            src_ref=cur_buf.at[pl.ds(pl.multiple_of(peer * band, band), band), :],
            dst_ref=rs_box.at[m],
            send_sem=x_send.at[0],
            recv_sem=x_recv.at[0],
            device_id=(peer, d),
            device_id_type=MESH,
        )

    def gather_copy(k):
        return pltpu.make_async_remote_copy(
            src_ref=slab,
            dst_ref=ens.at[m],
            send_sem=x_send.at[1],
            recv_sem=x_recv.at[1],
            device_id=((m + k) % n_mem, d),
            device_id_type=MESH,
        )

    steps = sorted(range(1, n_mem), key=lambda k: -min(k, n_mem - k))
    for k in steps:
        scatter_copy(k).start()
    rs_box[m] = cur_buf[pl.ds(pl.multiple_of(m * band, band), band), :]
    turn_mean(1)
    others = rs_box.at[pl.ds(0, n_mem - 1)]
    pltpu.make_async_copy(others, others, x_recv.at[0]).wait()
    total = jnp.sum(rs_box[...], axis=0)
    slab[...] = total
    for k in steps:
        gather_copy(k).start()
    ens[m] = total
    end_mean(1)
    p_out[...] = less_mean(current, mean_of(1, m) - mean_of(0, m))
    all_means = mean_of(1, 0) - mean_of(0, 0)
    for i in range(1, n_mem):
        all_means = all_means + (mean_of(1, i) - mean_of(0, i))
    others = ens.at[pl.ds(0, n_mem - 1)]
    pltpu.make_async_copy(others, others, x_recv.at[1]).wait()
    summed = jnp.concatenate([ens[i] for i in range(n_mem)], axis=0)
    e_out[...] = less_mean(summed, all_means) / n_mem

    pltpu.make_async_copy(snd, snd, s_send).wait()
    pltpu.make_async_copy(reach, reach, h_sem.at[0]).wait()
    sent = box_a.at[:, pl.ds(0, LINE - 1)]
    pltpu.make_async_copy(sent, sent, a_send).wait()
    sent = box_x.at[:, pl.ds(0, len(shifts))]
    pltpu.make_async_copy(sent, sent, b_send).wait()
    sent = ens.at[pl.ds(0, n_mem - 1)]
    for phase in range(2):
        pltpu.make_async_copy(sent, sent, x_send.at[phase]).wait()


def hand_over(p, t, e, p_out, t_out, e_out, sem):
    moves = [
        pltpu.make_async_copy(src, dst, sem.at[i])
        for i, (src, dst) in enumerate(((p, p_out.at[0]), (t, t_out.at[0]), (e, e_out)))
    ]
    for move in moves:
        move.start()
    for move in moves:
        move.wait()


def per_device(
    acoustic_perturbation,
    prior_acoustic_state,
    thermal_anomaly,
    model_parameters,
    crossing_velocity,
    face_extent,
    face_metric_factor,
    reciprocal_polygon_surface,
    owned_totals,
    export_lists,
    face_neighbour_pair,
    polygon_side_lookup,
):
    n_mem = lax.axis_size("member")
    n_line = lax.axis_size("dom") // LINE
    n_all = n_mem * n_line
    band = LV // n_mem
    vmem = pl.BlockSpec(memory_space=pltpu.VMEM)
    anyw = pl.BlockSpec(memory_space=pl.ANY)
    dma = pltpu.SemaphoreType.DMA
    held = pl.pallas_call(
        kernel,
        out_shape=tuple(pltpu.VMEM((LV, CC), F32) for _ in range(3)),
        in_specs=[anyw] * 10,
        out_specs=(vmem, vmem, vmem),
        scratch_shapes=[
            pltpu.SMEM((1, 4), F32),
            pltpu.VMEM((LV, CC), F32),
            pltpu.VMEM((LV, CC), F32),
            pltpu.VMEM((LV, CC), F32),
            pltpu.VMEM((LV, 3 * CC), F32),
            pltpu.VMEM((1, 3 * CC), F32),
            pltpu.VMEM((1, 3 * CC), F32),
            pltpu.VMEM((1, CC), F32),
            pltpu.VMEM((NBK, 1, HB), jnp.int32),
            pltpu.VMEM((2, 3 * CC), jnp.int32),
            pltpu.VMEM((3, EXT, CC), F8),
            pltpu.VMEM((CC, HALO), F8),
            pltpu.VMEM((3, LV, CC), F32),
            pltpu.VMEM((3, 8, CC), F32),
            pltpu.VMEM((8, NBK, LV, HB), F32),
            pltpu.VMEM((8, NBK, LV, HB), F32),
            pltpu.VMEM((NBK, 1, HB), F32),
            pltpu.VMEM((NBK, 1, HB), F32),
            pltpu.VMEM((2, 1, HB), F32),
            pltpu.VMEM((2, 1, HB), F32),
            pltpu.VMEM((2, LINE, 1, HB), F32),
            pltpu.VMEM((2, n_all, 1, HB), F32),
            pltpu.VMEM((LV, CC), F32),
            pltpu.VMEM((n_mem, band, CC), F32),
            pltpu.VMEM((band, CC), F32),
            pltpu.VMEM((n_mem, band, CC), F32),
            dma((10,)),
            dma,
            dma((8, 2)),
            dma((2,)),
            dma,
            dma((2,)),
            dma,
            dma((2,)),
            dma((2,)),
            dma((2,)),
        ],
        compiler_params=pltpu.CompilerParams(collective_id=0, has_side_effects=True),
    )(
        model_parameters,
        acoustic_perturbation,
        prior_acoustic_state,
        thermal_anomaly,
        crossing_velocity,
        face_extent[None, :],
        face_metric_factor[None, :],
        reciprocal_polygon_surface[None, :],
        export_lists.reshape(NBK, 1, HB),
        face_neighbour_pair,
    )
    return pl.pallas_call(
        hand_over,
        out_shape=(
            jax.ShapeDtypeStruct((1, LV, CC), F32),
            jax.ShapeDtypeStruct((1, LV, CC), F32),
            jax.ShapeDtypeStruct((LV, CC), F32),
        ),
        in_specs=[vmem] * 3,
        out_specs=(anyw, anyw, anyw),
        scratch_shapes=[dma((3,))],
    )(*[pltpu.with_memory_space_constraint(x, pltpu.VMEM) for x in held])


def solution(mesh):
    in_specs = (
        P("member", None, "dom"),
        P("member", None, "dom"),
        P("member", None, "dom"),
        P("member", None),
        P(None, "dom"),
        P("dom"),
        P("dom"),
        P("dom"),
        P("dom"),
        P("dom", None, None),
        P(None, "dom"),
        P(None, "dom"),
    )
    out_specs = (P("member", None, "dom"), P("member", None, "dom"), P(None, "dom"))
    return jax.shard_map(
        per_device, mesh=mesh, in_specs=in_specs, out_specs=out_specs, check_vma=False
    )
```

```python
import jax
import jax.numpy as jnp
from jax import lax
from jax.experimental import pallas as pl
from jax.experimental.pallas import tpu as pltpu
from jax.sharding import PartitionSpec as P

MESH = pl.DeviceIdType.MESH
F32 = jnp.float32
BF16 = jnp.bfloat16
F8 = jnp.float8_e4m3fn

LV = 32
CC = 1024
NBK = 6
HB = 128
HALO = NBK * HB
EXT = CC + HALO
LINE = 16
DT = 0.25
NS = 3
OFFSETS = [(b // 2 + 1) * (1 - 2 * (b % 2)) for b in range(NBK)]
SEND_ORDER = (4, 5, 2, 3, 0, 1)


def split2(x):
    hi = x.astype(BF16)
    lo = (x - hi.astype(F32)).astype(BF16)
    return hi, lo


def rows2(*fields):
    return jnp.concatenate([part for x in fields for part in split2(x)], axis=0)


def split3(x):
    a = x.astype(BF16)
    r = x - a.astype(F32)
    b = r.astype(BF16)
    c = (r - b.astype(F32)).astype(BF16)
    return a, b, c


def mm(a, b):
    return jnp.dot(a, b, preferred_element_type=F32)


def mm_t(a, b):
    return lax.dot_general(a, b, (((1,), (1,)), ((), ())), preferred_element_type=F32)


def fold(o, i=0):
    return o[2 * i * LV : (2 * i + 1) * LV] + o[(2 * i + 1) * LV : (2 * i + 2) * LV]


def kernel(
    par_hbm, p_hbm, q_hbm, t_hbm, v_hbm, len_hbm, met_hbm, inv_hbm, exp_hbm, end_hbm,
    p_out, t_out, e_out,
    par, p_in, q_in, t_in, v_in, len_in, met_in, inv_in, exp_in, end_in,
    sel, esel, vd, sd, snd, rcv, reach, reach_in, row_a, row_b, box_a, box_x, zsnd, zbox, cur_buf, rs_box, slab, ens,
    in_sem, s_send, s_recv, h_send, h_recv, z_send, z_recv, a_send, a_recv, b_send, b_recv, x_send, x_recv,
):
    n_mem = lax.axis_size("member")
    n_dom = lax.axis_size("dom")
    n_line = n_dom // LINE
    m = lax.axis_index("member")
    d = lax.axis_index("dom")
    line, pos = d // LINE, d % LINE

    sources = (exp_hbm, t_hbm.at[0], p_hbm.at[0], end_hbm, len_hbm, met_hbm, v_hbm, inv_hbm, par_hbm, q_hbm.at[0])
    targets = (exp_in, t_in, p_in, end_in, len_in, met_in, v_in, inv_in, par, q_in)
    groups = (0, 1, 1, 2, 2, 2, 3, 3, 3, 3)
    loads = [
        pltpu.make_async_copy(src, dst, in_sem.at[i]) for i, (src, dst) in enumerate(zip(sources, targets))
    ]
    for load in loads:
        load.start()

    neighbours = [(m, (d + off + n_dom) % n_dom) for off in OFFSETS]
    in_line = [(m, line * LINE + (pos + k) % LINE) for k in range(1, LINE)]
    shifts = [(i, k) for i in range(n_mem) for k in range(n_line) if i or k]
    across = [((m + i) % n_mem, (d + k * LINE) % n_dom) for i, k in shifts]

    barrier = pltpu.get_barrier_semaphore()
    peers = neighbours + in_line + across
    peers += [((m + i) % n_mem, p) for i in range(1, n_mem) for _, p in neighbours]
    for peer in peers:
        pl.semaphore_signal(barrier, inc=1, device_id=peer, device_id_type=MESH)

    def loaded(group):
        for load, its in zip(loads, groups):
            if its == group:
                load.wait()

    iota32 = lax.broadcasted_iota(jnp.int32, (32, HB), 0).astype(F32).astype(BF16)
    one = jnp.full((32, HB), 1.0, BF16)
    zero = jnp.full((32, HB), 0.0, BF16)

    def packed_row(row):
        return jnp.broadcast_to(jnp.clip(row, -1.0, 256.0), (32, HB)).astype(BF16)

    def hot(r, want):
        return jnp.where(iota32 + jnp.asarray(32.0 * r, BF16) == want, one, zero).astype(F8)

    er = lax.broadcasted_iota(jnp.int32, (3 * HB, 3 * HB), 0)
    ec = lax.broadcasted_iota(jnp.int32, (3 * HB, 3 * HB), 1)
    order = jnp.where(er == 3 * (ec % HB) + ec // HB, 1.0, 0.0).astype(F32).astype(BF16).astype(F8)
    loaded(0)

    def build_exports(t, carry):
        base = pl.multiple_of(t * 256, 256)
        for b in range(NBK):
            want = packed_row(exp_in[b].astype(F32) - (t * 256).astype(F32))
            for r in range(8):
                esel[pl.ds(base + 32 * r, 32), b * HB : (b + 1) * HB] = hot(r, want)
        return carry

    lax.fori_loop(0, CC // 256, build_exports, 0)

    def halo_copy(slot, b):
        return pltpu.make_async_remote_copy(
            src_ref=snd.at[slot, b],
            dst_ref=rcv.at[slot, b],
            send_sem=s_send,
            recv_sem=s_recv.at[slot],
            device_id=neighbours[b],
            device_id_type=MESH,
        )

    def export_and_send(*slots_and_fields):
        slots, fields = slots_and_fields[::2], slots_and_fields[1::2]
        o = mm(rows2(*fields), esel[...])
        for i, slot in enumerate(slots):
            values = fold(o, i)
            for b in range(NBK):
                snd[slot, b] = values[:, b * HB : (b + 1) * HB]
        if slots[0] == 6:
            pl.semaphore_wait(barrier, len(peers))
        for slot in slots:
            for b in SEND_ORDER:
                halo_copy(slot, b).start()
        return fold(o)

    def arrived(slot):
        pltpu.make_async_copy(rcv.at[slot], rcv.at[slot], s_recv.at[slot]).wait()
        return jnp.concatenate([rcv[slot, b] for b in range(NBK)], axis=1)

    loaded(1)
    theta = t_in[...]
    pres = p_in[...]
    export_and_send(6, theta, 0, pres)

    loaded(2)
    ends = end_in[1:2, :]
    smalls = [(ends // 256).astype(F32), (ends % 256).astype(F32)]
    smalls += [part.astype(F32) for row in (len_in, met_in) for part in split3(row[...])]
    smalls = jnp.concatenate(smalls + [jnp.zeros((8, 3 * CC), F32)], axis=0).astype(BF16)
    loaded(3)
    speed = par[0, 0]
    kappa = 0.5 * par[0, 1]
    mixing = 0.6 * par[0, 2]
    couple = par[0, 3]
    inv = inv_in[...]
    stacked = jnp.concatenate([rows2(v_in[...]), smalls], axis=0)
    for g in range(CC // HB):
        o = mm(stacked[:, g * 3 * HB : (g + 1) * 3 * HB], order)
        vel = fold(o)
        small = jnp.concatenate(
            [o[64:65], o[65:66], o[66:67] + o[67:68] + o[68:69], o[69:70] + o[70:71] + o[71:72], o[76:80]], axis=0
        )
        for j in range(3):
            vd[j, :, g * HB : (g + 1) * HB] = vel[:, j * HB : (j + 1) * HB]
            sd[j, :, g * HB : (g + 1) * HB] = small[:, j * HB : (j + 1) * HB]

    owned = sd[0, 0:1, :] < EXT // 256

    def build_tile(t, tf, base):
        for g in range(CC // HB):
            lanes = slice(g * HB, (g + 1) * HB)
            for j in range(3):
                want = packed_row((sd[j, 0:1, lanes] - tf) * 256.0 + sd[j, 1:2, lanes])
                for r in range(8):
                    sel[j, pl.ds(base + 32 * r, 32), lanes] = hot(r, want)

    def build(t, carry):
        build_tile(t, t.astype(F32), pl.multiple_of(t * 256, 256))
        return carry

    lax.fori_loop(0, CC // 256, build, 0)

    def coefficients(j):
        v = vd[j]
        length = sd[j, 2:3, :]
        return length * (jnp.maximum(v, 0.0) + kappa), length * (jnp.minimum(v, 0.0) - kappa)

    def weight(j):
        return sd[j, 3:4, :]

    def near(*fields, theta_last=False):
        spans, at = [], 0
        for field in fields:
            spans.append((at, field.shape[0]))
            at += 2 * field.shape[0]

        def part(o, i):
            first, rows = spans[i]
            return o[first : first + rows] + o[first + rows : first + 2 * rows]

        lhs = rows2(*fields)
        nets = [jnp.zeros_like(field) for field in fields]
        ends_of = [mm(lhs, sel[0, :CC, :]), None, None]
        for j in range(3):
            if j < 2:
                ends_of[j + 1] = mm(lhs, sel[j + 1, :CC, :])
            flows = []
            for i, field in enumerate(fields):
                if theta_last and i == len(fields) - 1:
                    start, end = coefficients(j)
                    flows.append(start * field + end * part(ends_of[j], i))
                else:
                    flows.append(weight(j) * (part(ends_of[j], i) - field))
            incoming = mm_t(rows2(*flows), sel[j, :CC, :])
            nets = [net + flow - part(incoming, i) for i, (net, flow) in enumerate(zip(nets, flows))]
        return nets

    def far_pressure(slot, net):
        lhs = rows2(arrived(slot))
        for j in range(3):
            net = net + weight(j) * fold(mm(lhs, sel[j, CC:, :]))
        return net

    def far_theta(slot, net):
        lhs = rows2(arrived(slot))
        for j in range(3):
            net = net + coefficients(j)[1] * fold(mm(lhs, sel[j, CC:, :]))
        return net

    def far_both(slot_p, net_p, slot_t, net_t):
        lhs = rows2(arrived(slot_p), arrived(slot_t))
        for j in range(3):
            o = mm(lhs, sel[j, CC:, :])
            net_p = net_p + weight(j) * fold(o, 0)
            net_t = net_t + coefficients(j)[1] * fold(o, 1)
        return net_p, net_t

    def advance_theta(th, net):
        up = jnp.concatenate([th[1:], th[LV - 1 :]], axis=0) - th
        down = th - jnp.concatenate([th[:1], th[: LV - 1]], axis=0)
        return jnp.where(owned, th + DT * (mixing * (up - down) - inv * net), th)

    scale = speed * inv

    def advance(p, q, net, force):
        return jnp.where(owned, 2.0 * p - q + scale * net + force, p), p

    area = jnp.where(owned, 1.0 / inv, 0.0)

    def by_lane(p, factor):
        return sum(
            p[:, g * HB : (g + 1) * HB] * factor[:, g * HB : (g + 1) * HB] for g in range(CC // HB)
        )

    def partial_row(total):
        spread = by_lane(jnp.ones((1, CC), F32), area)
        padded = jnp.concatenate([total, spread, jnp.zeros((HB - LV - 1, HB), F32)], axis=0)
        return jnp.sum(padded.T, axis=0, keepdims=True)

    def reach_copy(which, b):
        return pltpu.make_async_remote_copy(
            src_ref=reach.at[which, b],
            dst_ref=reach_in.at[which, b],
            send_sem=h_send,
            recv_sem=h_recv.at[which],
            device_id=(m, (d - OFFSETS[b] + n_dom) % n_dom),
            device_id_type=MESH,
        )

    def three_rows(row):
        parts = [part.astype(F32) for part in split3(row)]
        return jnp.concatenate(parts + [jnp.zeros((13, row.shape[1]), F32)], axis=0).astype(BF16)

    def send_reach(which, rows):
        total = jnp.zeros((16, HALO), F32)
        for j in range(3):
            total = total + mm_t(three_rows(rows[j]), sel[j, CC:, :])
        total = jnp.sum(total, axis=0, keepdims=True)
        for b in range(NBK):
            reach[which, b] = total[:, b * HB : (b + 1) * HB]
            reach_copy(which, b).start()

    def reached(which):
        pltpu.make_async_copy(reach_in.at[which], reach_in.at[which], h_recv.at[which]).wait()
        row = jnp.concatenate([reach_in[which, b] for b in range(NBK)], axis=1)
        return jnp.sum(mm_t(three_rows(row), esel[...]), axis=0, keepdims=True)

    def halo_weight(j):
        block = sd[j, 0:1, :]
        return jnp.where((block >= CC // 256) & (block < EXT // 256), weight(j), 0.0)

    def spread_row(row):
        return jnp.broadcast_to(row, (HB, HB)).T[:LV]

    def line_copy(which, k):
        return pltpu.make_async_remote_copy(
            src_ref=row_a.at[which],
            dst_ref=box_a.at[which, pos],
            send_sem=a_send,
            recv_sem=a_recv.at[which],
            device_id=in_line[k],
            device_id_type=MESH,
        )

    def wide_copy(which, n):
        return pltpu.make_async_remote_copy(
            src_ref=row_b.at[which],
            dst_ref=box_x.at[which, m * n_line + line],
            send_sem=b_send,
            recv_sem=b_recv.at[which],
            device_id=across[n],
            device_id_type=MESH,
        )

    def start_mean(which, total):
        row = partial_row(total)
        row_a[which] = row
        for k in range(LINE - 1):
            line_copy(which, k).start()
        box_a[which, pos] = row

    def turn_mean(which):
        others = box_a.at[which, pl.ds(0, LINE - 1)]
        pltpu.make_async_copy(others, others, a_recv.at[which]).wait()
        row = jnp.sum(box_a[which], axis=0)
        row_b[which] = row
        for n in range(len(shifts)):
            wide_copy(which, n).start()
        box_x[which, m * n_line + line] = row

    def end_mean(which):
        others = box_x.at[which, pl.ds(0, len(shifts))]
        pltpu.make_async_copy(others, others, b_recv.at[which]).wait()

    def mean_of(which, member):
        return level_mean(box_x[which, pl.ds(member * n_line, n_line)])

    def level_mean(rows):
        row = jnp.sum(rows, axis=0)
        return row / row[:, LV : LV + 1]

    def over_cells(mean):
        return jnp.where(owned, jnp.concatenate([spread_row(mean)] * (CC // HB), axis=1), 0.0)

    for t in range(CC // 256, EXT // 256):
        build_tile(t, float(t), t * 256)
    net, net_theta = near(pres, theta, theta_last=True)
    net, net_theta = far_both(0, net, 6, net_theta)
    theta_next = advance_theta(theta, net_theta)
    force = couple * (theta_next - theta) / NS
    theta = theta_next
    pres, prev = advance(pres, q_in[...], net, force)
    export_and_send(1, pres)
    export_and_send(7, theta)
    send_reach(0, [weight(j) for j in range(3)])
    (net,) = near(pres)
    pres, prev = advance(pres, prev, far_pressure(1, net), force)
    export_and_send(2, pres)
    net, net_theta = near(pres, theta, theta_last=True)
    once = reached(0) - halo_weight(0) - halo_weight(1) - halo_weight(2)
    scaled = jnp.where(owned, once * inv, 0.0)
    send_reach(1, [weight(j) * scaled for j in range(3)])
    pres, prev = advance(pres, prev, far_pressure(2, net), force)
    export_and_send(3, pres)
    start_mean(0, by_lane(pres, area))
    net, twice = near(pres, jnp.concatenate([scaled, jnp.zeros((7, CC), F32)], axis=0))
    twice = twice[0:1] + reached(1)
    theta_next = advance_theta(theta, far_theta(7, net_theta))
    force = couple * (theta_next - theta) / NS
    t_out[...] = theta_next
    by_p = 3.0 * area + speed * (4.0 * once + speed * twice)
    by_q = 2.0 * area + speed * once
    by_f = 3.0 * area + speed * once
    pres, prev = advance(pres, prev, far_pressure(3, net), force)
    export_and_send(4, pres)
    start_mean(1, by_lane(pres, by_p) - by_lane(prev, by_q) + by_lane(force, by_f))
    (net,) = near(pres)
    turn_mean(0)
    pres, prev = advance(pres, prev, far_pressure(4, net), force)

    band = LV // n_mem
    steps = sorted(range(1, n_mem), key=lambda k: -min(k, n_mem - k))

    def band_of(member):
        return pl.ds(pl.multiple_of(member * band, band), band)

    def sum_copy(k, b):
        peer = (m + k) % n_mem
        return pltpu.make_async_remote_copy(
            src_ref=zsnd.at[b, band_of(peer), :],
            dst_ref=zbox.at[m, b],
            send_sem=z_send,
            recv_sem=z_recv,
            device_id=(peer, neighbours[b][1]),
            device_id_type=MESH,
        )

    def scatter_copy(k):
        peer = (m + k) % n_mem
        return pltpu.make_async_remote_copy(
            src_ref=cur_buf.at[band_of(peer), :],
            dst_ref=rs_box.at[m],
            send_sem=x_send.at[0],
            recv_sem=x_recv.at[0],
            device_id=(peer, d),
            device_id_type=MESH,
        )

    def gather_copy(k):
        return pltpu.make_async_remote_copy(
            src_ref=slab,
            dst_ref=ens.at[m],
            send_sem=x_send.at[1],
            recv_sem=x_recv.at[1],
            device_id=((m + k) % n_mem, d),
            device_id_type=MESH,
        )

    values = speed * export_and_send(5, pres)
    for b in range(NBK):
        zsnd[b] = values[:, b * HB : (b + 1) * HB]
    for k in steps:
        for b in SEND_ORDER:
            sum_copy(k, b).start()
    (net,) = near(pres)
    cur_buf[...] = advance(pres, prev, net, force)[0]
    for k in steps:
        scatter_copy(k).start()
    rs_box[m] = cur_buf[band_of(m), :]
    turn_mean(1)
    far = far_pressure(5, jnp.zeros((LV, CC), F32))
    for b in range(NBK):
        zbox[m, b] = speed * rcv[5, b, band_of(m), :]
    others = rs_box.at[pl.ds(0, n_mem - 1)]
    pltpu.make_async_copy(others, others, x_recv.at[0]).wait()
    others = zbox.at[pl.ds(0, n_mem - 1)]
    pltpu.make_async_copy(others, others, z_recv).wait()
    lhs = rows2(jnp.sum(jnp.concatenate([zbox[:, b] for b in range(NBK)], axis=2), axis=0))
    total = jnp.zeros((band, CC), F32)
    for j in range(3):
        o = mm(lhs, sel[j, CC:, :])
        total = total + weight(j) * (o[:band] + o[band:])
    total = jnp.sum(rs_box[...], axis=0) + jnp.where(owned, inv * total, 0.0)
    slab[...] = total
    for k in steps:
        gather_copy(k).start()
    ens[m] = total
    pres = jnp.where(owned, cur_buf[...] + scale * far, pres)
    end_mean(0)
    first_means = [mean_of(0, i) for i in range(n_mem)]
    first_mean = mean_of(0, m)
    current = pres - over_cells(first_mean)
    lowered = over_cells(sum(first_means))
    end_mean(1)
    p_out[...] = current - over_cells(mean_of(1, m) - first_mean)
    all_means = mean_of(1, 0) - first_means[0]
    for i in range(1, n_mem):
        all_means = all_means + (mean_of(1, i) - first_means[i])
    all_means = over_cells(all_means)
    others = ens.at[pl.ds(0, n_mem - 1)]
    pltpu.make_async_copy(others, others, x_recv.at[1]).wait()
    summed = jnp.concatenate([ens[i] for i in range(n_mem)], axis=0) - lowered
    e_out[...] = (summed - all_means) / n_mem

    pltpu.make_async_copy(snd, snd, s_send).wait()
    pltpu.make_async_copy(reach, reach, h_send).wait()
    sent = zbox.at[pl.ds(0, n_mem - 1)]
    pltpu.make_async_copy(sent, sent, z_send).wait()
    sent = box_a.at[:, pl.ds(0, LINE - 1)]
    pltpu.make_async_copy(sent, sent, a_send).wait()
    sent = box_x.at[:, pl.ds(0, len(shifts))]
    pltpu.make_async_copy(sent, sent, b_send).wait()
    sent = ens.at[pl.ds(0, n_mem - 1)]
    for phase in range(2):
        pltpu.make_async_copy(sent, sent, x_send.at[phase]).wait()


def hand_over(p, t, e, p_out, t_out, e_out, sem):
    moves = [
        pltpu.make_async_copy(src, dst, sem.at[i])
        for i, (src, dst) in enumerate(((p, p_out.at[0]), (t, t_out.at[0]), (e, e_out)))
    ]
    for move in moves:
        move.start()
    for move in moves:
        move.wait()


def per_device(
    acoustic_perturbation,
    prior_acoustic_state,
    thermal_anomaly,
    model_parameters,
    crossing_velocity,
    face_extent,
    face_metric_factor,
    reciprocal_polygon_surface,
    owned_totals,
    export_lists,
    face_neighbour_pair,
    polygon_side_lookup,
):
    n_mem = lax.axis_size("member")
    n_line = lax.axis_size("dom") // LINE
    n_all = n_mem * n_line
    band = LV // n_mem
    vmem = pl.BlockSpec(memory_space=pltpu.VMEM)
    anyw = pl.BlockSpec(memory_space=pl.ANY)
    dma = pltpu.SemaphoreType.DMA
    held = pl.pallas_call(
        kernel,
        out_shape=tuple(pltpu.VMEM((LV, CC), F32) for _ in range(3)),
        in_specs=[anyw] * 10,
        out_specs=(vmem, vmem, vmem),
        scratch_shapes=[
            pltpu.SMEM((1, 4), F32),
            pltpu.VMEM((LV, CC), F32),
            pltpu.VMEM((LV, CC), F32),
            pltpu.VMEM((LV, CC), F32),
            pltpu.VMEM((LV, 3 * CC), F32),
            pltpu.VMEM((1, 3 * CC), F32),
            pltpu.VMEM((1, 3 * CC), F32),
            pltpu.VMEM((1, CC), F32),
            pltpu.VMEM((NBK, 1, HB), jnp.int32),
            pltpu.VMEM((2, 3 * CC), jnp.int32),
            pltpu.VMEM((3, EXT, CC), F8),
            pltpu.VMEM((CC, HALO), F8),
            pltpu.VMEM((3, LV, CC), F32),
            pltpu.VMEM((3, 8, CC), F32),
            pltpu.VMEM((8, NBK, LV, HB), F32),
            pltpu.VMEM((8, NBK, LV, HB), F32),
            pltpu.VMEM((2, NBK, 1, HB), F32),
            pltpu.VMEM((2, NBK, 1, HB), F32),
            pltpu.VMEM((2, 1, HB), F32),
            pltpu.VMEM((2, 1, HB), F32),
            pltpu.VMEM((2, LINE, 1, HB), F32),
            pltpu.VMEM((2, n_all, 1, HB), F32),
            pltpu.VMEM((NBK, LV, HB), F32),
            pltpu.VMEM((n_mem, NBK, band, HB), F32),
            pltpu.VMEM((LV, CC), F32),
            pltpu.VMEM((n_mem, band, CC), F32),
            pltpu.VMEM((band, CC), F32),
            pltpu.VMEM((n_mem, band, CC), F32),
            dma((10,)),
            dma,
            dma((8,)),
            dma,
            dma((2,)),
            dma,
            dma,
            dma,
            dma((2,)),
            dma,
            dma((2,)),
            dma((2,)),
            dma((2,)),
        ],
        compiler_params=pltpu.CompilerParams(collective_id=0, has_side_effects=True),
    )(
        model_parameters,
        acoustic_perturbation,
        prior_acoustic_state,
        thermal_anomaly,
        crossing_velocity,
        face_extent[None, :],
        face_metric_factor[None, :],
        reciprocal_polygon_surface[None, :],
        export_lists.reshape(NBK, 1, HB),
        face_neighbour_pair,
    )
    return pl.pallas_call(
        hand_over,
        out_shape=(
            jax.ShapeDtypeStruct((1, LV, CC), F32),
            jax.ShapeDtypeStruct((1, LV, CC), F32),
            jax.ShapeDtypeStruct((LV, CC), F32),
        ),
        in_specs=[vmem] * 3,
        out_specs=(anyw, anyw, anyw),
        scratch_shapes=[dma((3,))],
    )(*[pltpu.with_memory_space_constraint(x, pltpu.VMEM) for x in held])


def solution(mesh):
    in_specs = (
        P("member", None, "dom"),
        P("member", None, "dom"),
        P("member", None, "dom"),
        P("member", None),
        P(None, "dom"),
        P("dom"),
        P("dom"),
        P("dom"),
        P("dom"),
        P("dom", None, None),
        P(None, "dom"),
        P(None, "dom"),
    )
    out_specs = (P("member", None, "dom"), P("member", None, "dom"), P(None, "dom"))
    return jax.shard_map(
        per_device, mesh=mesh, in_specs=in_specs, out_specs=out_specs, check_vma=False
    )
```

```python
import jax
import jax.numpy as jnp
from jax import lax
from jax.experimental import pallas as pl
from jax.experimental.pallas import tpu as pltpu
from jax.sharding import PartitionSpec as P

MESH = pl.DeviceIdType.MESH
F32 = jnp.float32
BF16 = jnp.bfloat16
F8 = jnp.float8_e4m3fn

LV = 32
CC = 1024
NBK = 6
HB = 128
HALO = NBK * HB
EXT = CC + HALO
LINE = 16
DT = 0.25
NS = 3
OFFSETS = [(b // 2 + 1) * (1 - 2 * (b % 2)) for b in range(NBK)]
SEND_ORDER = (4, 5, 2, 3, 0, 1)


def split2(x):
    hi = x.astype(BF16)
    lo = (x - hi.astype(F32)).astype(BF16)
    return hi, lo


def rows2(*fields):
    return jnp.concatenate([part for x in fields for part in split2(x)], axis=0)


def split3(x):
    a = x.astype(BF16)
    r = x - a.astype(F32)
    b = r.astype(BF16)
    c = (r - b.astype(F32)).astype(BF16)
    return a, b, c


def mm(a, b):
    return jnp.dot(a, b, preferred_element_type=F32)


def mm_t(a, b):
    return lax.dot_general(a, b, (((1,), (1,)), ((), ())), preferred_element_type=F32)


def fold(o, i=0):
    return o[2 * i * LV : (2 * i + 1) * LV] + o[(2 * i + 1) * LV : (2 * i + 2) * LV]


def kernel(
    par_hbm, p_hbm, q_hbm, t_hbm, v_hbm, len_hbm, met_hbm, inv_hbm, exp_hbm, end_hbm,
    p_out, t_out, e_out,
    par, p_in, q_in, t_in, v_in, len_in, met_in, inv_in, exp_in, end_in,
    sel, esel, vd, sd, snd, rcv, reach, reach_in, row_a, row_b, box_a, box_x, zsnd, zbox, cur_buf, rs_box, slab, ens,
    in_sem, s_send, s_recv, h_send, h_recv, z_send, z_recv, token, a_send, a_recv, b_send, b_recv, x_send, x_recv,
):
    n_mem = lax.axis_size("member")
    n_dom = lax.axis_size("dom")
    n_line = n_dom // LINE
    m = lax.axis_index("member")
    d = lax.axis_index("dom")
    line, pos = d // LINE, d % LINE

    sources = (exp_hbm, t_hbm.at[0], p_hbm.at[0], end_hbm, len_hbm, met_hbm, v_hbm, inv_hbm, par_hbm, q_hbm.at[0])
    targets = (exp_in, t_in, p_in, end_in, len_in, met_in, v_in, inv_in, par, q_in)
    groups = (0, 1, 1, 2, 2, 2, 3, 3, 3, 3)
    loads = [
        pltpu.make_async_copy(src, dst, in_sem.at[i]) for i, (src, dst) in enumerate(zip(sources, targets))
    ]
    for load in loads:
        load.start()

    neighbours = [(m, (d + off + n_dom) % n_dom) for off in OFFSETS]
    in_line = [(m, line * LINE + (pos + k) % LINE) for k in range(1, LINE)]
    shifts = [(i, k) for i in range(n_mem) for k in range(n_line) if i or k]
    across = [((m + i) % n_mem, (d + k * LINE) % n_dom) for i, k in shifts]

    barrier = pltpu.get_barrier_semaphore()
    members = [((m + i) % n_mem, d) for i in range(1, n_mem)]
    peers = neighbours + [in_line[k - 1] for k in (1, 2, 3, LINE - 3, LINE - 2, LINE - 1)]
    peers += members + [(m, (d + k * LINE) % n_dom) for k in range(1, n_line)]
    for peer in peers:
        pl.semaphore_signal(barrier, inc=1, device_id=peer, device_id_type=MESH)

    def loaded(group):
        for load, its in zip(loads, groups):
            if its == group:
                load.wait()

    iota32 = lax.broadcasted_iota(jnp.int32, (32, HB), 0).astype(F32).astype(BF16)
    one = jnp.full((32, HB), 1.0, BF16)
    zero = jnp.full((32, HB), 0.0, BF16)

    def packed_row(row):
        return jnp.broadcast_to(jnp.clip(row, -1.0, 256.0), (32, HB)).astype(BF16)

    def hot(r, want):
        return jnp.where(iota32 + jnp.asarray(32.0 * r, BF16) == want, one, zero).astype(F8)

    er = lax.broadcasted_iota(jnp.int32, (3 * HB, 3 * HB), 0)
    ec = lax.broadcasted_iota(jnp.int32, (3 * HB, 3 * HB), 1)
    order = jnp.where(er == 3 * (ec % HB) + ec // HB, 1.0, 0.0).astype(F32).astype(BF16).astype(F8)
    loaded(0)

    def build_exports(t, carry):
        base = pl.multiple_of(t * 256, 256)
        for b in range(NBK):
            want = packed_row(exp_in[b].astype(F32) - (t * 256).astype(F32))
            for r in range(8):
                esel[pl.ds(base + 32 * r, 32), b * HB : (b + 1) * HB] = hot(r, want)
        return carry

    lax.fori_loop(0, CC // 256, build_exports, 0)

    def halo_copy(slot, b):
        return pltpu.make_async_remote_copy(
            src_ref=snd.at[slot, b],
            dst_ref=rcv.at[slot, b],
            send_sem=s_send,
            recv_sem=s_recv.at[slot],
            device_id=neighbours[b],
            device_id_type=MESH,
        )

    def stage(*slots_and_fields):
        slots, fields = slots_and_fields[::2], slots_and_fields[1::2]
        o = mm(rows2(*fields), esel[...])
        for i, slot in enumerate(slots):
            values = fold(o, i)
            for b in range(NBK):
                snd[slot, b] = values[:, b * HB : (b + 1) * HB]
        return fold(o)

    def start(slot):
        for b in SEND_ORDER:
            halo_copy(slot, b).start()

    def arrived(slot):
        pltpu.make_async_copy(rcv.at[slot], rcv.at[slot], s_recv.at[slot]).wait()
        return jnp.concatenate([rcv[slot, b] for b in range(NBK)], axis=1)

    loaded(1)
    theta = t_in[...]
    pres = p_in[...]
    stage(6, theta, 0, pres)
    pl.semaphore_wait(barrier, len(peers))
    start(6)
    start(0)
    for member in members:
        pl.semaphore_signal(token, inc=1, device_id=member, device_id_type=MESH)

    loaded(2)
    ends = end_in[1:2, :]
    smalls = [(ends // 256).astype(F32), (ends % 256).astype(F32)]
    smalls += [part.astype(F32) for row in (len_in, met_in) for part in split3(row[...])]
    smalls = jnp.concatenate(smalls + [jnp.zeros((8, 3 * CC), F32)], axis=0).astype(BF16)
    loaded(3)
    speed = par[0, 0]
    kappa = 0.5 * par[0, 1]
    mixing = 0.6 * par[0, 2]
    couple = par[0, 3]
    inv = inv_in[...]
    stacked = jnp.concatenate([rows2(v_in[...]), smalls], axis=0)
    for g in range(CC // HB):
        o = mm(stacked[:, g * 3 * HB : (g + 1) * 3 * HB], order)
        vel = fold(o)
        small = jnp.concatenate(
            [o[64:65], o[65:66], o[66:67] + o[67:68] + o[68:69], o[69:70] + o[70:71] + o[71:72], o[76:80]], axis=0
        )
        for j in range(3):
            vd[j, :, g * HB : (g + 1) * HB] = vel[:, j * HB : (j + 1) * HB]
            sd[j, :, g * HB : (g + 1) * HB] = small[:, j * HB : (j + 1) * HB]

    owned = sd[0, 0:1, :] < EXT // 256

    def build_tile(t, tf, base):
        for g in range(CC // HB):
            lanes = slice(g * HB, (g + 1) * HB)
            for j in range(3):
                want = packed_row((sd[j, 0:1, lanes] - tf) * 256.0 + sd[j, 1:2, lanes])
                for r in range(8):
                    sel[j, pl.ds(base + 32 * r, 32), lanes] = hot(r, want)

    def build(t, carry):
        build_tile(t, t.astype(F32), pl.multiple_of(t * 256, 256))
        return carry

    lax.fori_loop(0, CC // 256, build, 0)

    def coefficients(j):
        v = vd[j]
        length = sd[j, 2:3, :]
        return length * (jnp.maximum(v, 0.0) + kappa), length * (jnp.minimum(v, 0.0) - kappa)

    def weight(j):
        return sd[j, 3:4, :]

    def near(*fields, theta_last=False):
        spans, at = [], 0
        for field in fields:
            spans.append((at, field.shape[0]))
            at += 2 * field.shape[0]

        def part(o, i):
            first, rows = spans[i]
            return o[first : first + rows] + o[first + rows : first + 2 * rows]

        lhs = rows2(*fields)
        nets = [jnp.zeros_like(field) for field in fields]
        ends_of = [mm(lhs, sel[0, :CC, :]), None, None]
        for j in range(3):
            if j < 2:
                ends_of[j + 1] = mm(lhs, sel[j + 1, :CC, :])
            flows = []
            for i, field in enumerate(fields):
                if theta_last and i == len(fields) - 1:
                    start, end = coefficients(j)
                    flows.append(start * field + end * part(ends_of[j], i))
                else:
                    flows.append(weight(j) * (part(ends_of[j], i) - field))
            incoming = mm_t(rows2(*flows), sel[j, :CC, :])
            nets = [net + flow - part(incoming, i) for i, (net, flow) in enumerate(zip(nets, flows))]
        return nets

    def far_pressure(slot, net, late=None):
        lhs = rows2(arrived(slot))
        if late is not None:
            start(late)
        for j in range(3):
            net = net + weight(j) * fold(mm(lhs, sel[j, CC:, :]))
        return net

    def far_theta(slot, net):
        lhs = rows2(arrived(slot))
        for j in range(3):
            net = net + coefficients(j)[1] * fold(mm(lhs, sel[j, CC:, :]))
        return net

    def far_both(slot_p, net_p, slot_t, net_t):
        lhs = rows2(arrived(slot_p), arrived(slot_t))
        for j in range(3):
            o = mm(lhs, sel[j, CC:, :])
            net_p = net_p + weight(j) * fold(o, 0)
            net_t = net_t + coefficients(j)[1] * fold(o, 1)
        return net_p, net_t

    def advance_theta(th, net):
        up = jnp.concatenate([th[1:], th[LV - 1 :]], axis=0) - th
        down = th - jnp.concatenate([th[:1], th[: LV - 1]], axis=0)
        return jnp.where(owned, th + DT * (mixing * (up - down) - inv * net), th)

    scale = speed * inv

    def advance(p, q, net, force):
        return jnp.where(owned, 2.0 * p - q + scale * net + force, p), p

    area = jnp.where(owned, 1.0 / inv, 0.0)

    def by_lane(p, factor):
        return sum(
            p[:, g * HB : (g + 1) * HB] * factor[:, g * HB : (g + 1) * HB] for g in range(CC // HB)
        )

    def partial_row(total, later):
        spread = by_lane(jnp.ones((1, CC), F32), area)
        parts = [total, spread, jnp.zeros((LV - 1, HB), F32), later, jnp.zeros((LV, HB), F32)]
        return jnp.sum(jnp.concatenate(parts, axis=0).T, axis=0, keepdims=True)

    def reach_copy(which, b):
        return pltpu.make_async_remote_copy(
            src_ref=reach.at[which, b],
            dst_ref=reach_in.at[which, b],
            send_sem=h_send,
            recv_sem=h_recv.at[which],
            device_id=(m, (d - OFFSETS[b] + n_dom) % n_dom),
            device_id_type=MESH,
        )

    def three_rows(row):
        parts = [part.astype(F32) for part in split3(row)]
        return jnp.concatenate(parts + [jnp.zeros((13, row.shape[1]), F32)], axis=0).astype(BF16)

    def send_reach(which, rows):
        total = jnp.zeros((16, HALO), F32)
        for j in range(3):
            total = total + mm_t(three_rows(rows[j]), sel[j, CC:, :])
        total = jnp.sum(total, axis=0, keepdims=True)
        for b in range(NBK):
            reach[which, b] = total[:, b * HB : (b + 1) * HB]
            reach_copy(which, b).start()

    def reached(which):
        pltpu.make_async_copy(reach_in.at[which], reach_in.at[which], h_recv.at[which]).wait()
        row = jnp.concatenate([reach_in[which, b] for b in range(NBK)], axis=1)
        return jnp.sum(mm_t(three_rows(row), esel[...]), axis=0, keepdims=True)

    def halo_weight(j):
        block = sd[j, 0:1, :]
        return jnp.where((block >= CC // 256) & (block < EXT // 256), weight(j), 0.0)

    def line_copy(k):
        return pltpu.make_async_remote_copy(
            src_ref=row_a,
            dst_ref=box_a.at[pos],
            send_sem=a_send,
            recv_sem=a_recv,
            device_id=in_line[k],
            device_id_type=MESH,
        )

    def wide_copy(n):
        return pltpu.make_async_remote_copy(
            src_ref=row_b,
            dst_ref=box_x.at[m * n_line + line],
            send_sem=b_send,
            recv_sem=b_recv,
            device_id=across[n],
            device_id_type=MESH,
        )

    def start_means(row):
        row_a[...] = row
        for k in range(LINE - 1):
            line_copy(k).start()
        box_a[pos] = row

    def turn_means():
        others = box_a.at[pl.ds(0, LINE - 1)]
        pltpu.make_async_copy(others, others, a_recv).wait()
        row = jnp.sum(box_a[...], axis=0)
        row_b[...] = row
        for n in range(len(shifts)):
            wide_copy(n).start()
        box_x[m * n_line + line] = row

    def means_of(member):
        row = jnp.sum(box_x[pl.ds(member * n_line, n_line)], axis=0)
        return row / row[:, LV : LV + 1]

    def over_cells(column):
        return jnp.where(owned, jnp.concatenate([column] * (CC // HB), axis=1), 0.0)

    def both_means(row):
        columns = jnp.broadcast_to(row, (HB, HB)).T
        first = columns[:LV]
        return over_cells(first), over_cells(columns[2 * LV : 3 * LV] - first)

    for t in range(CC // 256, EXT // 256):
        build_tile(t, float(t), t * 256)
    net, net_theta = near(pres, theta, theta_last=True)
    net, net_theta = far_both(0, net, 6, net_theta)
    theta_next = advance_theta(theta, net_theta)
    force = couple * (theta_next - theta) / NS
    theta = theta_next
    pres, prev = advance(pres, q_in[...], net, force)
    stage(1, pres)
    start(1)
    stage(7, theta)
    send_reach(0, [weight(j) for j in range(3)])
    (net,) = near(pres)
    pres, prev = advance(pres, prev, far_pressure(1, net, late=7), force)
    stage(2, pres)
    start(2)
    net, net_theta = near(pres, theta, theta_last=True)
    once = reached(0) - halo_weight(0) - halo_weight(1) - halo_weight(2)
    scaled = jnp.where(owned, once * inv, 0.0)
    send_reach(1, [weight(j) * scaled for j in range(3)])
    pres, prev = advance(pres, prev, far_pressure(2, net), force)
    stage(3, pres)
    start(3)
    first_sums = by_lane(pres, area)
    net, twice = near(pres, jnp.concatenate([scaled, jnp.zeros((7, CC), F32)], axis=0))
    twice = twice[0:1] + reached(1)
    theta_next = advance_theta(theta, far_theta(7, net_theta))
    force = couple * (theta_next - theta) / NS
    t_out[...] = theta_next
    by_p = 3.0 * area + speed * (4.0 * once + speed * twice)
    by_q = 2.0 * area + speed * once
    by_f = 3.0 * area + speed * once
    pres, prev = advance(pres, prev, far_pressure(3, net), force)
    stage(4, pres)
    start(4)
    later_sums = by_lane(pres, by_p) - by_lane(prev, by_q) + by_lane(force, by_f)
    start_means(partial_row(first_sums, later_sums))
    (net,) = near(pres)
    pres, prev = advance(pres, prev, far_pressure(4, net), force)

    band = LV // n_mem
    steps = sorted(range(1, n_mem), key=lambda k: -min(k, n_mem - k))

    def band_of(member):
        return pl.ds(pl.multiple_of(member * band, band), band)

    def sum_copy(k, b):
        peer = (m + k) % n_mem
        return pltpu.make_async_remote_copy(
            src_ref=zsnd.at[b, band_of(peer), :],
            dst_ref=zbox.at[m, b],
            send_sem=z_send,
            recv_sem=z_recv,
            device_id=(peer, neighbours[b][1]),
            device_id_type=MESH,
        )

    def scatter_copy(k):
        peer = (m + k) % n_mem
        return pltpu.make_async_remote_copy(
            src_ref=cur_buf.at[band_of(peer), :],
            dst_ref=rs_box.at[m],
            send_sem=x_send.at[0],
            recv_sem=x_recv.at[0],
            device_id=(peer, d),
            device_id_type=MESH,
        )

    def gather_copy(k):
        return pltpu.make_async_remote_copy(
            src_ref=slab,
            dst_ref=ens.at[m],
            send_sem=x_send.at[1],
            recv_sem=x_recv.at[1],
            device_id=((m + k) % n_mem, d),
            device_id_type=MESH,
        )

    values = speed * stage(5, pres)
    start(5)
    for b in range(NBK):
        zsnd[b] = values[:, b * HB : (b + 1) * HB]
    pl.semaphore_wait(token, n_mem - 1)
    for k in steps:
        for b in SEND_ORDER:
            sum_copy(k, b).start()
    (net,) = near(pres)
    cur_buf[...] = advance(pres, prev, net, force)[0]
    for k in steps:
        scatter_copy(k).start()
    rs_box[m] = cur_buf[band_of(m), :]
    turn_means()
    far = far_pressure(5, jnp.zeros((LV, CC), F32))
    for b in range(NBK):
        zbox[m, b] = speed * rcv[5, b, band_of(m), :]
    others = rs_box.at[pl.ds(0, n_mem - 1)]
    pltpu.make_async_copy(others, others, x_recv.at[0]).wait()
    others = zbox.at[pl.ds(0, n_mem - 1)]
    pltpu.make_async_copy(others, others, z_recv).wait()
    lhs = rows2(jnp.sum(jnp.concatenate([zbox[:, b] for b in range(NBK)], axis=2), axis=0))
    total = jnp.zeros((band, CC), F32)
    for j in range(3):
        o = mm(lhs, sel[j, CC:, :])
        total = total + weight(j) * (o[:band] + o[band:])
    total = jnp.sum(rs_box[...], axis=0) + jnp.where(owned, inv * total, 0.0)
    slab[...] = total
    for k in steps:
        gather_copy(k).start()
    ens[m] = total
    pres = jnp.where(owned, cur_buf[...] + scale * far, pres)
    others = box_x.at[pl.ds(0, len(shifts))]
    pltpu.make_async_copy(others, others, b_recv).wait()
    first, second = both_means(means_of(m))
    p_out[...] = (pres - first) - second
    first, second = both_means(sum(means_of(i) for i in range(n_mem)))
    others = ens.at[pl.ds(0, n_mem - 1)]
    pltpu.make_async_copy(others, others, x_recv.at[1]).wait()
    summed = jnp.concatenate([ens[i] for i in range(n_mem)], axis=0)
    e_out[...] = ((summed - first) - second) / n_mem

    pltpu.make_async_copy(snd, snd, s_send).wait()
    pltpu.make_async_copy(reach, reach, h_send).wait()
    sent = zbox.at[pl.ds(0, n_mem - 1)]
    pltpu.make_async_copy(sent, sent, z_send).wait()
    sent = box_a.at[pl.ds(0, LINE - 1)]
    pltpu.make_async_copy(sent, sent, a_send).wait()
    sent = box_x.at[pl.ds(0, len(shifts))]
    pltpu.make_async_copy(sent, sent, b_send).wait()
    sent = ens.at[pl.ds(0, n_mem - 1)]
    for phase in range(2):
        pltpu.make_async_copy(sent, sent, x_send.at[phase]).wait()


def hand_over(p, t, e, p_out, t_out, e_out, sem):
    moves = [
        pltpu.make_async_copy(src, dst, sem.at[i])
        for i, (src, dst) in enumerate(((p, p_out.at[0]), (t, t_out.at[0]), (e, e_out)))
    ]
    for move in moves:
        move.start()
    for move in moves:
        move.wait()


def per_device(
    acoustic_perturbation,
    prior_acoustic_state,
    thermal_anomaly,
    model_parameters,
    crossing_velocity,
    face_extent,
    face_metric_factor,
    reciprocal_polygon_surface,
    owned_totals,
    export_lists,
    face_neighbour_pair,
    polygon_side_lookup,
):
    n_mem = lax.axis_size("member")
    n_line = lax.axis_size("dom") // LINE
    n_all = n_mem * n_line
    band = LV // n_mem
    vmem = pl.BlockSpec(memory_space=pltpu.VMEM)
    anyw = pl.BlockSpec(memory_space=pl.ANY)
    dma = pltpu.SemaphoreType.DMA
    held = pl.pallas_call(
        kernel,
        out_shape=tuple(pltpu.VMEM((LV, CC), F32) for _ in range(3)),
        in_specs=[anyw] * 10,
        out_specs=(vmem, vmem, vmem),
        scratch_shapes=[
            pltpu.SMEM((1, 4), F32),
            pltpu.VMEM((LV, CC), F32),
            pltpu.VMEM((LV, CC), F32),
            pltpu.VMEM((LV, CC), F32),
            pltpu.VMEM((LV, 3 * CC), F32),
            pltpu.VMEM((1, 3 * CC), F32),
            pltpu.VMEM((1, 3 * CC), F32),
            pltpu.VMEM((1, CC), F32),
            pltpu.VMEM((NBK, 1, HB), jnp.int32),
            pltpu.VMEM((2, 3 * CC), jnp.int32),
            pltpu.VMEM((3, EXT, CC), F8),
            pltpu.VMEM((CC, HALO), F8),
            pltpu.VMEM((3, LV, CC), F32),
            pltpu.VMEM((3, 8, CC), F32),
            pltpu.VMEM((8, NBK, LV, HB), F32),
            pltpu.VMEM((8, NBK, LV, HB), F32),
            pltpu.VMEM((2, NBK, 1, HB), F32),
            pltpu.VMEM((2, NBK, 1, HB), F32),
            pltpu.VMEM((1, HB), F32),
            pltpu.VMEM((1, HB), F32),
            pltpu.VMEM((LINE, 1, HB), F32),
            pltpu.VMEM((n_all, 1, HB), F32),
            pltpu.VMEM((NBK, LV, HB), F32),
            pltpu.VMEM((n_mem, NBK, band, HB), F32),
            pltpu.VMEM((LV, CC), F32),
            pltpu.VMEM((n_mem, band, CC), F32),
            pltpu.VMEM((band, CC), F32),
            pltpu.VMEM((n_mem, band, CC), F32),
            dma((10,)),
            dma,
            dma((8,)),
            dma,
            dma((2,)),
            dma,
            dma,
            pltpu.SemaphoreType.REGULAR,
            dma,
            dma,
            dma,
            dma,
            dma((2,)),
            dma((2,)),
        ],
        compiler_params=pltpu.CompilerParams(collective_id=0, has_side_effects=True),
    )(
        model_parameters,
        acoustic_perturbation,
        prior_acoustic_state,
        thermal_anomaly,
        crossing_velocity,
        face_extent[None, :],
        face_metric_factor[None, :],
        reciprocal_polygon_surface[None, :],
        export_lists.reshape(NBK, 1, HB),
        face_neighbour_pair,
    )
    return pl.pallas_call(
        hand_over,
        out_shape=(
            jax.ShapeDtypeStruct((1, LV, CC), F32),
            jax.ShapeDtypeStruct((1, LV, CC), F32),
            jax.ShapeDtypeStruct((LV, CC), F32),
        ),
        in_specs=[vmem] * 3,
        out_specs=(anyw, anyw, anyw),
        scratch_shapes=[dma((3,))],
    )(*[pltpu.with_memory_space_constraint(x, pltpu.VMEM) for x in held])


def solution(mesh):
    in_specs = (
        P("member", None, "dom"),
        P("member", None, "dom"),
        P("member", None, "dom"),
        P("member", None),
        P(None, "dom"),
        P("dom"),
        P("dom"),
        P("dom"),
        P("dom"),
        P("dom", None, None),
        P(None, "dom"),
        P(None, "dom"),
    )
    out_specs = (P("member", None, "dom"), P("member", None, "dom"), P(None, "dom"))
    return jax.shard_map(
        per_device, mesh=mesh, in_specs=in_specs, out_specs=out_specs, check_vma=False
    )
```

```python
import jax
import jax.numpy as jnp
from jax import lax
from jax.experimental import pallas as pl
from jax.experimental.pallas import tpu as pltpu
from jax.sharding import PartitionSpec as P

MESH = pl.DeviceIdType.MESH
F32 = jnp.float32
BF16 = jnp.bfloat16
F8 = jnp.float8_e4m3fn

LV = 32
CC = 1024
NBK = 6
HB = 128
HALO = NBK * HB
EXT = CC + HALO
LINE = 16
DT = 0.25
NS = 3
OFFSETS = [(b // 2 + 1) * (1 - 2 * (b % 2)) for b in range(NBK)]
SEND_ORDER = (4, 5, 2, 3, 0, 1)


def split2(x):
    hi = x.astype(BF16)
    lo = (x - hi.astype(F32)).astype(BF16)
    return hi, lo


def rows2(*fields):
    return jnp.concatenate([part for x in fields for part in split2(x)], axis=0)


def split3(x):
    a = x.astype(BF16)
    r = x - a.astype(F32)
    b = r.astype(BF16)
    c = (r - b.astype(F32)).astype(BF16)
    return a, b, c


def mm(a, b):
    return jnp.dot(a, b, preferred_element_type=F32)


def mm_t(a, b):
    return lax.dot_general(a, b, (((1,), (1,)), ((), ())), preferred_element_type=F32)


def fold(o, i=0):
    return o[2 * i * LV : (2 * i + 1) * LV] + o[(2 * i + 1) * LV : (2 * i + 2) * LV]


def kernel(
    par_hbm, p_hbm, q_hbm, t_hbm, v_hbm, len_hbm, met_hbm, inv_hbm, exp_hbm, end_hbm,
    p_out, t_out, e_out,
    par, p_in, q_in, t_in, v_in, len_in, met_in, inv_in, exp_in, end_in,
    sel, esel, vd, sd, snd, rcv, reach, reach_in, row_a, row_b, box_a, box_x, zsnd, zbox, cur_buf, rs_box, slab, ens,
    in_sem, s_send, s_recv, h_send, h_recv, z_send, z_recv, token, a_send, a_recv, b_send, b_recv, x_send, x_recv,
):
    n_mem = lax.axis_size("member")
    n_dom = lax.axis_size("dom")
    n_line = n_dom // LINE
    m = lax.axis_index("member")
    d = lax.axis_index("dom")
    line, pos = d // LINE, d % LINE

    neighbours = [(m, (d + off + n_dom) % n_dom) for off in OFFSETS]
    in_line = [(m, line * LINE + (pos + k) % LINE) for k in range(1, LINE)]
    shifts = [(i, k) for i in range(n_mem) for k in range(n_line) if i or k]
    across = [((m + i) % n_mem, (d + k * LINE) % n_dom) for i, k in shifts]

    barrier = pltpu.get_barrier_semaphore()
    for peer in neighbours:
        pl.semaphore_signal(barrier, inc=1, device_id=peer, device_id_type=MESH)

    sources = (exp_hbm, t_hbm.at[0], p_hbm.at[0], end_hbm, len_hbm, met_hbm, v_hbm, inv_hbm, par_hbm, q_hbm.at[0])
    targets = (exp_in, t_in, p_in, end_in, len_in, met_in, v_in, inv_in, par, q_in)
    groups = (0, 1, 1, 2, 2, 2, 3, 3, 3, 3)
    loads = [
        pltpu.make_async_copy(src, dst, in_sem.at[i]) for i, (src, dst) in enumerate(zip(sources, targets))
    ]
    for load in loads:
        load.start()

    members = [((m + i) % n_mem, d) for i in range(1, n_mem)]
    peers = neighbours + [in_line[k - 1] for k in (1, 2, 3, LINE - 3, LINE - 2, LINE - 1)]
    peers += members + [(m, (d + k * LINE) % n_dom) for k in range(1, n_line)]
    for peer in peers[len(neighbours) :]:
        pl.semaphore_signal(barrier, inc=1, device_id=peer, device_id_type=MESH)

    def loaded(group):
        for load, its in zip(loads, groups):
            if its == group:
                load.wait()

    iota32 = lax.broadcasted_iota(jnp.int32, (32, HB), 0).astype(F32).astype(BF16)
    one = jnp.full((32, HB), 1.0, BF16)
    zero = jnp.full((32, HB), 0.0, BF16)

    def packed_row(row):
        return jnp.broadcast_to(jnp.clip(row, -1.0, 256.0), (32, HB)).astype(BF16)

    def hot(r, want):
        return jnp.where(iota32 + jnp.asarray(32.0 * r, BF16) == want, one, zero).astype(F8)

    er = lax.broadcasted_iota(jnp.int32, (3 * HB, 3 * HB), 0)
    ec = lax.broadcasted_iota(jnp.int32, (3 * HB, 3 * HB), 1)
    order = jnp.where(er == 3 * (ec % HB) + ec // HB, 1.0, 0.0).astype(F32).astype(BF16).astype(F8)
    loaded(0)

    def build_exports(t, carry):
        base = pl.multiple_of(t * 256, 256)
        for b in range(NBK):
            want = packed_row(exp_in[b].astype(F32) - (t * 256).astype(F32))
            for r in range(8):
                esel[pl.ds(base + 32 * r, 32), b * HB : (b + 1) * HB] = hot(r, want)
        return carry

    lax.fori_loop(0, CC // 256, build_exports, 0)

    def halo_copy(slot, b):
        return pltpu.make_async_remote_copy(
            src_ref=snd.at[slot, b],
            dst_ref=rcv.at[slot, b],
            send_sem=s_send,
            recv_sem=s_recv.at[slot],
            device_id=neighbours[b],
            device_id_type=MESH,
        )

    def stage(*slots_and_fields):
        slots, fields = slots_and_fields[::2], slots_and_fields[1::2]
        o = mm(rows2(*fields), esel[...])
        for i, slot in enumerate(slots):
            values = fold(o, i)
            for b in range(NBK):
                snd[slot, b] = values[:, b * HB : (b + 1) * HB]
        return fold(o)

    def start(slot):
        for b in SEND_ORDER:
            halo_copy(slot, b).start()

    def arrived(slot):
        pltpu.make_async_copy(rcv.at[slot], rcv.at[slot], s_recv.at[slot]).wait()
        return jnp.concatenate([rcv[slot, b] for b in range(NBK)], axis=1)

    loaded(1)
    theta = t_in[...]
    pres = p_in[...]
    stage(6, theta, 0, pres)
    pl.semaphore_wait(barrier, len(peers))
    start(6)
    start(0)
    for member in members:
        pl.semaphore_signal(token, inc=1, device_id=member, device_id_type=MESH)

    loaded(2)
    ends = end_in[1:2, :]
    smalls = [(ends // 256).astype(F32), (ends % 256).astype(F32)]
    smalls += [part.astype(F32) for row in (len_in, met_in) for part in split3(row[...])]
    smalls = jnp.concatenate(smalls + [jnp.zeros((8, 3 * CC), F32)], axis=0).astype(BF16)
    loaded(3)
    speed = par[0, 0]
    kappa = 0.5 * par[0, 1]
    mixing = 0.6 * par[0, 2]
    couple = par[0, 3]
    inv = inv_in[...]
    stacked = jnp.concatenate([rows2(v_in[...]), smalls], axis=0)
    for g in range(CC // HB):
        o = mm(stacked[:, g * 3 * HB : (g + 1) * 3 * HB], order)
        vel = fold(o)
        small = jnp.concatenate(
            [o[64:65], o[65:66], o[66:67] + o[67:68] + o[68:69], o[69:70] + o[70:71] + o[71:72], o[76:80]], axis=0
        )
        for j in range(3):
            vd[j, :, g * HB : (g + 1) * HB] = vel[:, j * HB : (j + 1) * HB]
            sd[j, :, g * HB : (g + 1) * HB] = small[:, j * HB : (j + 1) * HB]

    owned = sd[0, 0:1, :] < EXT // 256

    def build_tile(t, tf, base):
        for g in range(CC // HB):
            lanes = slice(g * HB, (g + 1) * HB)
            for j in range(3):
                want = packed_row((sd[j, 0:1, lanes] - tf) * 256.0 + sd[j, 1:2, lanes])
                for r in range(8):
                    sel[j, pl.ds(base + 32 * r, 32), lanes] = hot(r, want)

    def build(t, carry):
        build_tile(t, t.astype(F32), pl.multiple_of(t * 256, 256))
        return carry

    lax.fori_loop(0, CC // 256, build, 0)

    def coefficients(j):
        v = vd[j]
        length = sd[j, 2:3, :]
        return length * (jnp.maximum(v, 0.0) + kappa), length * (jnp.minimum(v, 0.0) - kappa)

    def weight(j):
        return sd[j, 3:4, :]

    def near(*fields, theta_last=False):
        spans, at = [], 0
        for field in fields:
            spans.append((at, field.shape[0]))
            at += 2 * field.shape[0]

        def part(o, i):
            first, rows = spans[i]
            return o[first : first + rows] + o[first + rows : first + 2 * rows]

        lhs = rows2(*fields)
        nets = [jnp.zeros_like(field) for field in fields]
        ends_of = [mm(lhs, sel[0, :CC, :]), None, None]
        for j in range(3):
            if j < 2:
                ends_of[j + 1] = mm(lhs, sel[j + 1, :CC, :])
            flows = []
            for i, field in enumerate(fields):
                if theta_last and i == len(fields) - 1:
                    start, end = coefficients(j)
                    flows.append(start * field + end * part(ends_of[j], i))
                else:
                    flows.append(weight(j) * (part(ends_of[j], i) - field))
            incoming = mm_t(rows2(*flows), sel[j, :CC, :])
            nets = [net + flow - part(incoming, i) for i, (net, flow) in enumerate(zip(nets, flows))]
        return nets

    def far_pressure(slot, net, late=None):
        lhs = rows2(arrived(slot))
        if late is not None:
            start(late)
        for j in range(3):
            net = net + weight(j) * fold(mm(lhs, sel[j, CC:, :]))
        return net

    def far_theta(slot, net):
        lhs = rows2(arrived(slot))
        for j in range(3):
            net = net + coefficients(j)[1] * fold(mm(lhs, sel[j, CC:, :]))
        return net

    def far_both(slot_p, net_p, slot_t, net_t):
        lhs = rows2(arrived(slot_p), arrived(slot_t))
        for j in range(3):
            o = mm(lhs, sel[j, CC:, :])
            net_p = net_p + weight(j) * fold(o, 0)
            net_t = net_t + coefficients(j)[1] * fold(o, 1)
        return net_p, net_t

    def advance_theta(th, net):
        up = jnp.concatenate([th[1:], th[LV - 1 :]], axis=0) - th
        down = th - jnp.concatenate([th[:1], th[: LV - 1]], axis=0)
        return jnp.where(owned, th + DT * (mixing * (up - down) - inv * net), th)

    scale = speed * inv

    def advance(p, q, net, force):
        return jnp.where(owned, 2.0 * p - q + scale * net + force, p), p

    area = jnp.where(owned, 1.0 / inv, 0.0)

    def by_lane(p, factor):
        return sum(
            p[:, g * HB : (g + 1) * HB] * factor[:, g * HB : (g + 1) * HB] for g in range(CC // HB)
        )

    def partial_row(total, later):
        spread = by_lane(jnp.ones((1, CC), F32), area)
        parts = [total, spread, jnp.zeros((LV - 1, HB), F32), later, jnp.zeros((LV, HB), F32)]
        return jnp.sum(jnp.concatenate(parts, axis=0).T, axis=0, keepdims=True)

    def reach_copy(which, b):
        return pltpu.make_async_remote_copy(
            src_ref=reach.at[which, b],
            dst_ref=reach_in.at[which, b],
            send_sem=h_send,
            recv_sem=h_recv.at[which],
            device_id=(m, (d - OFFSETS[b] + n_dom) % n_dom),
            device_id_type=MESH,
        )

    def three_rows(row):
        parts = [part.astype(F32) for part in split3(row)]
        return jnp.concatenate(parts + [jnp.zeros((13, row.shape[1]), F32)], axis=0).astype(BF16)

    def send_reach(which, rows):
        total = jnp.zeros((16, HALO), F32)
        for j in range(3):
            total = total + mm_t(three_rows(rows[j]), sel[j, CC:, :])
        total = jnp.sum(total, axis=0, keepdims=True)
        for b in range(NBK):
            reach[which, b] = total[:, b * HB : (b + 1) * HB]
            reach_copy(which, b).start()

    def reached(which):
        pltpu.make_async_copy(reach_in.at[which], reach_in.at[which], h_recv.at[which]).wait()
        row = jnp.concatenate([reach_in[which, b] for b in range(NBK)], axis=1)
        return jnp.sum(mm_t(three_rows(row), esel[...]), axis=0, keepdims=True)

    def halo_weight(j):
        block = sd[j, 0:1, :]
        return jnp.where((block >= CC // 256) & (block < EXT // 256), weight(j), 0.0)

    def line_copy(k):
        return pltpu.make_async_remote_copy(
            src_ref=row_a,
            dst_ref=box_a.at[pos],
            send_sem=a_send,
            recv_sem=a_recv,
            device_id=in_line[k],
            device_id_type=MESH,
        )

    def wide_copy(n):
        return pltpu.make_async_remote_copy(
            src_ref=row_b,
            dst_ref=box_x.at[m * n_line + line],
            send_sem=b_send,
            recv_sem=b_recv,
            device_id=across[n],
            device_id_type=MESH,
        )

    def start_means(row):
        row_a[...] = row
        for k in range(LINE - 1):
            line_copy(k).start()
        box_a[pos] = row

    def turn_means():
        others = box_a.at[pl.ds(0, LINE - 1)]
        pltpu.make_async_copy(others, others, a_recv).wait()
        row = jnp.sum(box_a[...], axis=0)
        row_b[...] = row
        for n in range(len(shifts)):
            wide_copy(n).start()
        box_x[m * n_line + line] = row

    def means_of(member):
        row = jnp.sum(box_x[pl.ds(member * n_line, n_line)], axis=0)
        return row / row[:, LV : LV + 1]

    def over_cells(column):
        return jnp.where(owned, jnp.concatenate([column] * (CC // HB), axis=1), 0.0)

    def both_means(row):
        columns = jnp.broadcast_to(row, (HB, HB)).T
        first = columns[:LV]
        return over_cells(first), over_cells(columns[2 * LV : 3 * LV] - first)

    for t in range(CC // 256, EXT // 256):
        build_tile(t, float(t), t * 256)
    net, net_theta = near(pres, theta, theta_last=True)
    net, net_theta = far_both(0, net, 6, net_theta)
    theta_next = advance_theta(theta, net_theta)
    force = couple * (theta_next - theta) / NS
    theta = theta_next
    pres, prev = advance(pres, q_in[...], net, force)
    stage(1, pres)
    start(1)
    stage(7, theta)
    send_reach(0, [weight(j) for j in range(3)])
    (net,) = near(pres)
    pres, prev = advance(pres, prev, far_pressure(1, net, late=7), force)
    stage(2, pres)
    start(2)
    net, net_theta = near(pres, theta, theta_last=True)
    once = reached(0) - halo_weight(0) - halo_weight(1) - halo_weight(2)
    scaled = jnp.where(owned, once * inv, 0.0)
    send_reach(1, [weight(j) * scaled for j in range(3)])
    pres, prev = advance(pres, prev, far_pressure(2, net), force)
    stage(3, pres)
    start(3)
    first_sums = by_lane(pres, area)
    net, twice = near(pres, jnp.concatenate([scaled, jnp.zeros((7, CC), F32)], axis=0))
    twice = twice[0:1] + reached(1)
    theta_next = advance_theta(theta, far_theta(7, net_theta))
    force = couple * (theta_next - theta) / NS
    t_out[...] = theta_next
    by_p = 3.0 * area + speed * (4.0 * once + speed * twice)
    by_q = 2.0 * area + speed * once
    by_f = 3.0 * area + speed * once
    pres, prev = advance(pres, prev, far_pressure(3, net), force)
    stage(4, pres)
    start(4)
    later_sums = by_lane(pres, by_p) - by_lane(prev, by_q) + by_lane(force, by_f)
    start_means(partial_row(first_sums, later_sums))
    (net,) = near(pres)
    pres, prev = advance(pres, prev, far_pressure(4, net), force)

    band = LV // n_mem
    steps = sorted(range(1, n_mem), key=lambda k: -min(k, n_mem - k))

    def band_of(member):
        return pl.ds(pl.multiple_of(member * band, band), band)

    def sum_copy(k, b):
        peer = (m + k) % n_mem
        return pltpu.make_async_remote_copy(
            src_ref=zsnd.at[b, band_of(peer), :],
            dst_ref=zbox.at[m, b],
            send_sem=z_send,
            recv_sem=z_recv,
            device_id=(peer, neighbours[b][1]),
            device_id_type=MESH,
        )

    def scatter_copy(k):
        peer = (m + k) % n_mem
        return pltpu.make_async_remote_copy(
            src_ref=cur_buf.at[band_of(peer), :],
            dst_ref=rs_box.at[m],
            send_sem=x_send.at[0],
            recv_sem=x_recv.at[0],
            device_id=(peer, d),
            device_id_type=MESH,
        )

    def gather_copy(k):
        return pltpu.make_async_remote_copy(
            src_ref=slab,
            dst_ref=ens.at[m],
            send_sem=x_send.at[1],
            recv_sem=x_recv.at[1],
            device_id=((m + k) % n_mem, d),
            device_id_type=MESH,
        )

    values = speed * stage(5, pres)
    for b in range(NBK):
        zsnd[b] = values[:, b * HB : (b + 1) * HB]
    pl.semaphore_wait(token, n_mem - 1)
    for k in steps:
        for b in SEND_ORDER:
            sum_copy(k, b).start()
    start(5)
    (net,) = near(pres)
    cur_buf[...] = advance(pres, prev, net, force)[0]
    for k in steps:
        scatter_copy(k).start()
    rs_box[m] = cur_buf[band_of(m), :]
    turn_means()
    far = far_pressure(5, jnp.zeros((LV, CC), F32))
    for b in range(NBK):
        zbox[m, b] = speed * rcv[5, b, band_of(m), :]
    others = rs_box.at[pl.ds(0, n_mem - 1)]
    pltpu.make_async_copy(others, others, x_recv.at[0]).wait()
    others = zbox.at[pl.ds(0, n_mem - 1)]
    pltpu.make_async_copy(others, others, z_recv).wait()
    lhs = rows2(jnp.sum(jnp.concatenate([zbox[:, b] for b in range(NBK)], axis=2), axis=0))
    total = jnp.zeros((band, CC), F32)
    for j in range(3):
        o = mm(lhs, sel[j, CC:, :])
        total = total + weight(j) * (o[:band] + o[band:])
    total = jnp.sum(rs_box[...], axis=0) + jnp.where(owned, inv * total, 0.0)
    slab[...] = total
    for k in steps:
        gather_copy(k).start()
    ens[m] = total
    pres = jnp.where(owned, cur_buf[...] + scale * far, pres)
    others = box_x.at[pl.ds(0, len(shifts))]
    pltpu.make_async_copy(others, others, b_recv).wait()
    first, second = both_means(means_of(m))
    p_out[...] = (pres - first) - second
    first, second = both_means(sum(means_of(i) for i in range(n_mem)))
    others = ens.at[pl.ds(0, n_mem - 1)]
    pltpu.make_async_copy(others, others, x_recv.at[1]).wait()
    summed = jnp.concatenate([ens[i] for i in range(n_mem)], axis=0)
    e_out[...] = ((summed - first) - second) / n_mem

    pltpu.make_async_copy(snd, snd, s_send).wait()
    pltpu.make_async_copy(reach, reach, h_send).wait()
    sent = zbox.at[pl.ds(0, n_mem - 1)]
    pltpu.make_async_copy(sent, sent, z_send).wait()
    sent = box_a.at[pl.ds(0, LINE - 1)]
    pltpu.make_async_copy(sent, sent, a_send).wait()
    sent = box_x.at[pl.ds(0, len(shifts))]
    pltpu.make_async_copy(sent, sent, b_send).wait()
    sent = ens.at[pl.ds(0, n_mem - 1)]
    for phase in range(2):
        pltpu.make_async_copy(sent, sent, x_send.at[phase]).wait()


def hand_over(p, t, e, p_out, t_out, e_out, sem):
    moves = [
        pltpu.make_async_copy(src, dst, sem.at[i])
        for i, (src, dst) in enumerate(((p, p_out.at[0]), (t, t_out.at[0]), (e, e_out)))
    ]
    for move in moves:
        move.start()
    for move in moves:
        move.wait()


def per_device(
    acoustic_perturbation,
    prior_acoustic_state,
    thermal_anomaly,
    model_parameters,
    crossing_velocity,
    face_extent,
    face_metric_factor,
    reciprocal_polygon_surface,
    owned_totals,
    export_lists,
    face_neighbour_pair,
    polygon_side_lookup,
):
    n_mem = lax.axis_size("member")
    n_line = lax.axis_size("dom") // LINE
    n_all = n_mem * n_line
    band = LV // n_mem
    vmem = pl.BlockSpec(memory_space=pltpu.VMEM)
    anyw = pl.BlockSpec(memory_space=pl.ANY)
    dma = pltpu.SemaphoreType.DMA
    held = pl.pallas_call(
        kernel,
        out_shape=tuple(pltpu.VMEM((LV, CC), F32) for _ in range(3)),
        in_specs=[anyw] * 10,
        out_specs=(vmem, vmem, vmem),
        scratch_shapes=[
            pltpu.SMEM((1, 4), F32),
            pltpu.VMEM((LV, CC), F32),
            pltpu.VMEM((LV, CC), F32),
            pltpu.VMEM((LV, CC), F32),
            pltpu.VMEM((LV, 3 * CC), F32),
            pltpu.VMEM((1, 3 * CC), F32),
            pltpu.VMEM((1, 3 * CC), F32),
            pltpu.VMEM((1, CC), F32),
            pltpu.VMEM((NBK, 1, HB), jnp.int32),
            pltpu.VMEM((2, 3 * CC), jnp.int32),
            pltpu.VMEM((3, EXT, CC), F8),
            pltpu.VMEM((CC, HALO), F8),
            pltpu.VMEM((3, LV, CC), F32),
            pltpu.VMEM((3, 8, CC), F32),
            pltpu.VMEM((8, NBK, LV, HB), F32),
            pltpu.VMEM((8, NBK, LV, HB), F32),
            pltpu.VMEM((2, NBK, 1, HB), F32),
            pltpu.VMEM((2, NBK, 1, HB), F32),
            pltpu.VMEM((1, HB), F32),
            pltpu.VMEM((1, HB), F32),
            pltpu.VMEM((LINE, 1, HB), F32),
            pltpu.VMEM((n_all, 1, HB), F32),
            pltpu.VMEM((NBK, LV, HB), F32),
            pltpu.VMEM((n_mem, NBK, band, HB), F32),
            pltpu.VMEM((LV, CC), F32),
            pltpu.VMEM((n_mem, band, CC), F32),
            pltpu.VMEM((band, CC), F32),
            pltpu.VMEM((n_mem, band, CC), F32),
            dma((10,)),
            dma,
            dma((8,)),
            dma,
            dma((2,)),
            dma,
            dma,
            pltpu.SemaphoreType.REGULAR,
            dma,
            dma,
            dma,
            dma,
            dma((2,)),
            dma((2,)),
        ],
        compiler_params=pltpu.CompilerParams(collective_id=0, has_side_effects=True),
    )(
        model_parameters,
        acoustic_perturbation,
        prior_acoustic_state,
        thermal_anomaly,
        crossing_velocity,
        face_extent[None, :],
        face_metric_factor[None, :],
        reciprocal_polygon_surface[None, :],
        export_lists.reshape(NBK, 1, HB),
        face_neighbour_pair,
    )
    return pl.pallas_call(
        hand_over,
        out_shape=(
            jax.ShapeDtypeStruct((1, LV, CC), F32),
            jax.ShapeDtypeStruct((1, LV, CC), F32),
            jax.ShapeDtypeStruct((LV, CC), F32),
        ),
        in_specs=[vmem] * 3,
        out_specs=(anyw, anyw, anyw),
        scratch_shapes=[dma((3,))],
    )(*[pltpu.with_memory_space_constraint(x, pltpu.VMEM) for x in held])


def solution(mesh):
    in_specs = (
        P("member", None, "dom"),
        P("member", None, "dom"),
        P("member", None, "dom"),
        P("member", None),
        P(None, "dom"),
        P("dom"),
        P("dom"),
        P("dom"),
        P("dom"),
        P("dom", None, None),
        P(None, "dom"),
        P(None, "dom"),
    )
    out_specs = (P("member", None, "dom"), P("member", None, "dom"), P(None, "dom"))
    return jax.shard_map(
        per_device, mesh=mesh, in_specs=in_specs, out_specs=out_specs, check_vma=False
    )
```

```python
import jax
import jax.numpy as jnp
from jax import lax
from jax.experimental import pallas as pl
from jax.experimental.pallas import tpu as pltpu
from jax.sharding import PartitionSpec as P

MESH = pl.DeviceIdType.MESH
F32 = jnp.float32
BF16 = jnp.bfloat16
F8 = jnp.float8_e4m3fn

LV = 32
CC = 1024
NBK = 6
HB = 128
HALO = NBK * HB
EXT = CC + HALO
LINE = 16
DT = 0.25
NS = 3
OFFSETS = [(b // 2 + 1) * (1 - 2 * (b % 2)) for b in range(NBK)]
SEND_ORDER = (4, 5, 0, 1, 2, 3)


def split2(x):
    hi = x.astype(BF16)
    lo = (x - hi.astype(F32)).astype(BF16)
    return hi, lo


def rows2(*fields):
    return jnp.concatenate([part for x in fields for part in split2(x)], axis=0)


def split3(x):
    a = x.astype(BF16)
    r = x - a.astype(F32)
    b = r.astype(BF16)
    c = (r - b.astype(F32)).astype(BF16)
    return a, b, c


def mm(a, b):
    return jnp.dot(a, b, preferred_element_type=F32)


def mm_t(a, b):
    return lax.dot_general(a, b, (((1,), (1,)), ((), ())), preferred_element_type=F32)


def fold(o, i=0):
    return o[2 * i * LV : (2 * i + 1) * LV] + o[(2 * i + 1) * LV : (2 * i + 2) * LV]


def kernel(
    par_hbm, p_hbm, q_hbm, t_hbm, v_hbm, len_hbm, met_hbm, inv_hbm, exp_hbm, end_hbm,
    p_out, t_out, e_out,
    par, p_in, q_in, t_in, v_in, len_in, met_in, inv_in, exp_in, end_in,
    sel, esel, vd, sd, snd, rcv, reach, reach_in, row_a, row_b, box_a, box_x, zsnd, zbox, cur_buf, rs_box, slab, ens,
    in_sem, s_send, s_recv, h_send, h_recv, z_send, z_recv, token, a_send, a_recv, b_send, b_recv, x_send, x_recv,
):
    n_mem = lax.axis_size("member")
    n_dom = lax.axis_size("dom")
    n_line = n_dom // LINE
    m = lax.axis_index("member")
    d = lax.axis_index("dom")
    line, pos = d // LINE, d % LINE

    neighbours = [(m, (d + off + n_dom) % n_dom) for off in OFFSETS]
    in_line = [(m, line * LINE + (pos + k) % LINE) for k in range(1, LINE)]
    shifts = [(i, k) for i in range(n_mem) for k in range(n_line) if i or k]
    across = [((m + i) % n_mem, (d + k * LINE) % n_dom) for i, k in shifts]

    barrier = pltpu.get_barrier_semaphore()
    for peer in neighbours:
        pl.semaphore_signal(barrier, inc=1, device_id=peer, device_id_type=MESH)

    sources = (exp_hbm, t_hbm.at[0], p_hbm.at[0], end_hbm, len_hbm, met_hbm, v_hbm, inv_hbm, par_hbm, q_hbm.at[0])
    targets = (exp_in, t_in, p_in, end_in, len_in, met_in, v_in, inv_in, par, q_in)
    groups = (0, 1, 1, 2, 2, 2, 3, 3, 3, 3)
    loads = [
        pltpu.make_async_copy(src, dst, in_sem.at[i]) for i, (src, dst) in enumerate(zip(sources, targets))
    ]
    for load in loads:
        load.start()

    members = [((m + i) % n_mem, d) for i in range(1, n_mem)]
    peers = neighbours + [in_line[k - 1] for k in (1, 2, 3, LINE - 3, LINE - 2, LINE - 1)]
    peers += members + [(m, (d + k * LINE) % n_dom) for k in range(1, n_line)]
    for peer in peers[len(neighbours) :]:
        pl.semaphore_signal(barrier, inc=1, device_id=peer, device_id_type=MESH)

    def loaded(group):
        for load, its in zip(loads, groups):
            if its == group:
                load.wait()

    iota32 = lax.broadcasted_iota(jnp.int32, (32, HB), 0).astype(F32).astype(BF16)
    one = jnp.full((32, HB), 1.0, BF16)
    zero = jnp.full((32, HB), 0.0, BF16)

    def packed_row(row):
        return jnp.broadcast_to(jnp.clip(row, -1.0, 256.0), (32, HB)).astype(BF16)

    def hot(r, want):
        return jnp.where(iota32 + jnp.asarray(32.0 * r, BF16) == want, one, zero).astype(F8)

    er = lax.broadcasted_iota(jnp.int32, (3 * HB, 3 * HB), 0)
    ec = lax.broadcasted_iota(jnp.int32, (3 * HB, 3 * HB), 1)
    order = jnp.where(er == 3 * (ec % HB) + ec // HB, 1.0, 0.0).astype(F32).astype(BF16).astype(F8)
    loaded(0)

    def build_exports(t, carry):
        base = pl.multiple_of(t * 256, 256)
        for b in range(NBK):
            want = packed_row(exp_in[b].astype(F32) - (t * 256).astype(F32))
            for r in range(8):
                esel[pl.ds(base + 32 * r, 32), b * HB : (b + 1) * HB] = hot(r, want)
        return carry

    lax.fori_loop(0, CC // 256, build_exports, 0)

    def halo_copy(slot, b):
        return pltpu.make_async_remote_copy(
            src_ref=snd.at[slot, b],
            dst_ref=rcv.at[slot, b],
            send_sem=s_send,
            recv_sem=s_recv.at[slot],
            device_id=neighbours[b],
            device_id_type=MESH,
        )

    def stage(*slots_and_fields):
        slots, fields = slots_and_fields[::2], slots_and_fields[1::2]
        o = mm(rows2(*fields), esel[...])
        for i, slot in enumerate(slots):
            values = fold(o, i)
            for b in range(NBK):
                snd[slot, b] = values[:, b * HB : (b + 1) * HB]
        return fold(o)

    def start(slot):
        for b in SEND_ORDER:
            halo_copy(slot, b).start()

    def arrived(slot):
        pltpu.make_async_copy(rcv.at[slot], rcv.at[slot], s_recv.at[slot]).wait()
        return jnp.concatenate([rcv[slot, b] for b in range(NBK)], axis=1)

    loaded(1)
    theta = t_in[...]
    pres = p_in[...]
    stage(6, theta, 0, pres)
    pl.semaphore_wait(barrier, len(peers))
    start(6)
    start(0)
    for member in members:
        pl.semaphore_signal(token, inc=1, device_id=member, device_id_type=MESH)

    loaded(2)
    ends = end_in[1:2, :]
    smalls = [(ends // 256).astype(F32), (ends % 256).astype(F32)]
    smalls += [part.astype(F32) for row in (len_in, met_in) for part in split3(row[...])]
    smalls = jnp.concatenate(smalls + [jnp.zeros((8, 3 * CC), F32)], axis=0).astype(BF16)
    loaded(3)
    speed = par[0, 0]
    kappa = 0.5 * par[0, 1]
    mixing = 0.6 * par[0, 2]
    couple = par[0, 3]
    inv = inv_in[...]
    stacked = jnp.concatenate([rows2(v_in[...]), smalls], axis=0)
    for g in range(CC // HB):
        o = mm(stacked[:, g * 3 * HB : (g + 1) * 3 * HB], order)
        vel = fold(o)
        small = jnp.concatenate(
            [o[64:65], o[65:66], o[66:67] + o[67:68] + o[68:69], o[69:70] + o[70:71] + o[71:72], o[76:80]], axis=0
        )
        for j in range(3):
            vd[j, :, g * HB : (g + 1) * HB] = vel[:, j * HB : (j + 1) * HB]
            sd[j, :, g * HB : (g + 1) * HB] = small[:, j * HB : (j + 1) * HB]

    owned = sd[0, 0:1, :] < EXT // 256

    def build_tile(t, tf, base):
        for g in range(CC // HB):
            lanes = slice(g * HB, (g + 1) * HB)
            for j in range(3):
                want = packed_row((sd[j, 0:1, lanes] - tf) * 256.0 + sd[j, 1:2, lanes])
                for r in range(8):
                    sel[j, pl.ds(base + 32 * r, 32), lanes] = hot(r, want)

    def build(t, carry):
        build_tile(t, t.astype(F32), pl.multiple_of(t * 256, 256))
        return carry

    lax.fori_loop(0, CC // 256, build, 0)

    def coefficients(j):
        v = vd[j]
        length = sd[j, 2:3, :]
        return length * (jnp.maximum(v, 0.0) + kappa), length * (jnp.minimum(v, 0.0) - kappa)

    def weight(j):
        return sd[j, 3:4, :]

    def near(*fields, theta_last=False):
        spans, at = [], 0
        for field in fields:
            spans.append((at, field.shape[0]))
            at += 2 * field.shape[0]

        def part(o, i):
            first, rows = spans[i]
            return o[first : first + rows] + o[first + rows : first + 2 * rows]

        lhs = rows2(*fields)
        nets = [jnp.zeros_like(field) for field in fields]
        ends_of = [mm(lhs, sel[0, :CC, :]), None, None]
        for j in range(3):
            if j < 2:
                ends_of[j + 1] = mm(lhs, sel[j + 1, :CC, :])
            flows = []
            for i, field in enumerate(fields):
                if theta_last and i == len(fields) - 1:
                    start, end = coefficients(j)
                    flows.append(start * field + end * part(ends_of[j], i))
                else:
                    flows.append(weight(j) * (part(ends_of[j], i) - field))
            incoming = mm_t(rows2(*flows), sel[j, :CC, :])
            nets = [net + flow - part(incoming, i) for i, (net, flow) in enumerate(zip(nets, flows))]
        return nets

    def far_pressure(slot, net, late=None):
        lhs = rows2(arrived(slot))
        if late is not None:
            start(late)
        for j in range(3):
            net = net + weight(j) * fold(mm(lhs, sel[j, CC:, :]))
        return net

    def far_theta(slot, net):
        lhs = rows2(arrived(slot))
        for j in range(3):
            net = net + coefficients(j)[1] * fold(mm(lhs, sel[j, CC:, :]))
        return net

    def advance_theta(th, net):
        up = jnp.concatenate([th[1:], th[LV - 1 :]], axis=0) - th
        down = th - jnp.concatenate([th[:1], th[: LV - 1]], axis=0)
        return jnp.where(owned, th + DT * (mixing * (up - down) - inv * net), th)

    scale = speed * inv

    def advance(p, q, net, force):
        return jnp.where(owned, 2.0 * p - q + scale * net + force, p), p

    area = jnp.where(owned, 1.0 / inv, 0.0)

    def by_lane(p, factor):
        return sum(
            p[:, g * HB : (g + 1) * HB] * factor[:, g * HB : (g + 1) * HB] for g in range(CC // HB)
        )

    def partial_row(total, later):
        spread = by_lane(jnp.ones((1, CC), F32), area)
        parts = [total, spread, jnp.zeros((LV - 1, HB), F32), later, jnp.zeros((LV, HB), F32)]
        return jnp.sum(jnp.concatenate(parts, axis=0).T, axis=0, keepdims=True)

    def reach_copy(which, b):
        return pltpu.make_async_remote_copy(
            src_ref=reach.at[which, b],
            dst_ref=reach_in.at[which, b],
            send_sem=h_send,
            recv_sem=h_recv.at[which],
            device_id=(m, (d - OFFSETS[b] + n_dom) % n_dom),
            device_id_type=MESH,
        )

    def three_rows(row):
        parts = [part.astype(F32) for part in split3(row)]
        return jnp.concatenate(parts + [jnp.zeros((13, row.shape[1]), F32)], axis=0).astype(BF16)

    def send_reach(which, rows):
        total = jnp.zeros((16, HALO), F32)
        for j in range(3):
            total = total + mm_t(three_rows(rows[j]), sel[j, CC:, :])
        total = jnp.sum(total, axis=0, keepdims=True)
        for b in range(NBK):
            reach[which, b] = total[:, b * HB : (b + 1) * HB]
            reach_copy(which, b).start()

    def reached(which):
        pltpu.make_async_copy(reach_in.at[which], reach_in.at[which], h_recv.at[which]).wait()
        row = jnp.concatenate([reach_in[which, b] for b in range(NBK)], axis=1)
        return jnp.sum(mm_t(three_rows(row), esel[...]), axis=0, keepdims=True)

    def halo_weight(j):
        block = sd[j, 0:1, :]
        return jnp.where((block >= CC // 256) & (block < EXT // 256), weight(j), 0.0)

    def line_copy(k):
        return pltpu.make_async_remote_copy(
            src_ref=row_a,
            dst_ref=box_a.at[pos],
            send_sem=a_send,
            recv_sem=a_recv,
            device_id=in_line[k],
            device_id_type=MESH,
        )

    def wide_copy(n):
        return pltpu.make_async_remote_copy(
            src_ref=row_b,
            dst_ref=box_x.at[m * n_line + line],
            send_sem=b_send,
            recv_sem=b_recv,
            device_id=across[n],
            device_id_type=MESH,
        )

    def start_means(row):
        row_a[...] = row
        for k in range(LINE - 1):
            line_copy(k).start()
        box_a[pos] = row

    def turn_means():
        others = box_a.at[pl.ds(0, LINE - 1)]
        pltpu.make_async_copy(others, others, a_recv).wait()
        row = jnp.sum(box_a[...], axis=0)
        row_b[...] = row
        for n in range(len(shifts)):
            wide_copy(n).start()
        box_x[m * n_line + line] = row

    def means_of(member):
        row = jnp.sum(box_x[pl.ds(member * n_line, n_line)], axis=0)
        return row / row[:, LV : LV + 1]

    def over_cells(column):
        return jnp.where(owned, jnp.concatenate([column] * (CC // HB), axis=1), 0.0)

    def both_means(row):
        columns = jnp.broadcast_to(row, (HB, HB)).T
        first = columns[:LV]
        return over_cells(first), over_cells(columns[2 * LV : 3 * LV] - first)

    for t in range(CC // 256, EXT // 256):
        build_tile(t, float(t), t * 256)
    net, net_theta = near(pres, theta, theta_last=True)
    theta_next = advance_theta(theta, far_theta(6, net_theta))
    force = couple * (theta_next - theta) / NS
    theta = theta_next
    pres, prev = advance(pres, q_in[...], far_pressure(0, net), force)
    stage(1, pres)
    start(1)
    stage(7, theta)
    send_reach(0, [weight(j) for j in range(3)])
    (net,) = near(pres)
    pres, prev = advance(pres, prev, far_pressure(1, net, late=7), force)
    stage(2, pres)
    start(2)
    net, net_theta = near(pres, theta, theta_last=True)
    once = reached(0) - halo_weight(0) - halo_weight(1) - halo_weight(2)
    scaled = jnp.where(owned, once * inv, 0.0)
    send_reach(1, [weight(j) * scaled for j in range(3)])
    pres, prev = advance(pres, prev, far_pressure(2, net), force)
    stage(3, pres)
    start(3)
    first_sums = by_lane(pres, area)
    net, twice = near(pres, jnp.concatenate([scaled, jnp.zeros((7, CC), F32)], axis=0))
    twice = twice[0:1] + reached(1)
    theta_next = advance_theta(theta, far_theta(7, net_theta))
    force = couple * (theta_next - theta) / NS
    t_out[...] = theta_next
    by_p = 3.0 * area + speed * (4.0 * once + speed * twice)
    by_q = 2.0 * area + speed * once
    by_f = 3.0 * area + speed * once
    pres, prev = advance(pres, prev, far_pressure(3, net), force)
    stage(4, pres)
    start(4)
    later_sums = by_lane(pres, by_p) - by_lane(prev, by_q) + by_lane(force, by_f)
    start_means(partial_row(first_sums, later_sums))
    (net,) = near(pres)
    pres, prev = advance(pres, prev, far_pressure(4, net), force)

    band = LV // n_mem
    steps = sorted(range(1, n_mem), key=lambda k: -min(k, n_mem - k))

    def band_of(member):
        return pl.ds(pl.multiple_of(member * band, band), band)

    def sum_copy(k, b):
        peer = (m + k) % n_mem
        return pltpu.make_async_remote_copy(
            src_ref=zsnd.at[b, band_of(peer), :],
            dst_ref=zbox.at[m, b],
            send_sem=z_send,
            recv_sem=z_recv,
            device_id=(peer, neighbours[b][1]),
            device_id_type=MESH,
        )

    def scatter_copy(k):
        peer = (m + k) % n_mem
        return pltpu.make_async_remote_copy(
            src_ref=cur_buf.at[band_of(peer), :],
            dst_ref=rs_box.at[m],
            send_sem=x_send.at[0],
            recv_sem=x_recv.at[0],
            device_id=(peer, d),
            device_id_type=MESH,
        )

    def gather_copy(k):
        return pltpu.make_async_remote_copy(
            src_ref=slab,
            dst_ref=ens.at[m],
            send_sem=x_send.at[1],
            recv_sem=x_recv.at[1],
            device_id=((m + k) % n_mem, d),
            device_id_type=MESH,
        )

    values = speed * stage(5, pres)
    for b in range(NBK):
        zsnd[b] = values[:, b * HB : (b + 1) * HB]
    pl.semaphore_wait(token, n_mem - 1)
    for k in steps:
        for b in SEND_ORDER:
            sum_copy(k, b).start()
    start(5)
    (net,) = near(pres)
    cur_buf[...] = advance(pres, prev, net, force)[0]
    for k in steps:
        scatter_copy(k).start()
    rs_box[m] = cur_buf[band_of(m), :]
    turn_means()
    far = far_pressure(5, jnp.zeros((LV, CC), F32))
    for b in range(NBK):
        zbox[m, b] = speed * rcv[5, b, band_of(m), :]
    others = rs_box.at[pl.ds(0, n_mem - 1)]
    pltpu.make_async_copy(others, others, x_recv.at[0]).wait()
    others = zbox.at[pl.ds(0, n_mem - 1)]
    pltpu.make_async_copy(others, others, z_recv).wait()
    lhs = rows2(jnp.sum(jnp.concatenate([zbox[:, b] for b in range(NBK)], axis=2), axis=0))
    total = jnp.zeros((band, CC), F32)
    for j in range(3):
        o = mm(lhs, sel[j, CC:, :])
        total = total + weight(j) * (o[:band] + o[band:])
    total = jnp.sum(rs_box[...], axis=0) + jnp.where(owned, inv * total, 0.0)
    slab[...] = total
    for k in steps:
        gather_copy(k).start()
    ens[m] = total
    pres = jnp.where(owned, cur_buf[...] + scale * far, pres)
    others = box_x.at[pl.ds(0, len(shifts))]
    pltpu.make_async_copy(others, others, b_recv).wait()
    first, second = both_means(means_of(m))
    p_out[...] = (pres - first) - second
    first, second = both_means(sum(means_of(i) for i in range(n_mem)))
    others = ens.at[pl.ds(0, n_mem - 1)]
    pltpu.make_async_copy(others, others, x_recv.at[1]).wait()
    summed = jnp.concatenate([ens[i] for i in range(n_mem)], axis=0)
    e_out[...] = ((summed - first) - second) / n_mem

    pltpu.make_async_copy(snd, snd, s_send).wait()
    pltpu.make_async_copy(reach, reach, h_send).wait()
    sent = zbox.at[pl.ds(0, n_mem - 1)]
    pltpu.make_async_copy(sent, sent, z_send).wait()
    sent = box_a.at[pl.ds(0, LINE - 1)]
    pltpu.make_async_copy(sent, sent, a_send).wait()
    sent = box_x.at[pl.ds(0, len(shifts))]
    pltpu.make_async_copy(sent, sent, b_send).wait()
    sent = ens.at[pl.ds(0, n_mem - 1)]
    for phase in range(2):
        pltpu.make_async_copy(sent, sent, x_send.at[phase]).wait()


def hand_over(p, t, e, p_out, t_out, e_out, sem):
    moves = [
        pltpu.make_async_copy(src, dst, sem.at[i])
        for i, (src, dst) in enumerate(((p, p_out.at[0]), (t, t_out.at[0]), (e, e_out)))
    ]
    for move in moves:
        move.start()
    for move in moves:
        move.wait()


def per_device(
    acoustic_perturbation,
    prior_acoustic_state,
    thermal_anomaly,
    model_parameters,
    crossing_velocity,
    face_extent,
    face_metric_factor,
    reciprocal_polygon_surface,
    owned_totals,
    export_lists,
    face_neighbour_pair,
    polygon_side_lookup,
):
    n_mem = lax.axis_size("member")
    n_line = lax.axis_size("dom") // LINE
    n_all = n_mem * n_line
    band = LV // n_mem
    vmem = pl.BlockSpec(memory_space=pltpu.VMEM)
    anyw = pl.BlockSpec(memory_space=pl.ANY)
    dma = pltpu.SemaphoreType.DMA
    held = pl.pallas_call(
        kernel,
        out_shape=tuple(pltpu.VMEM((LV, CC), F32) for _ in range(3)),
        in_specs=[anyw] * 10,
        out_specs=(vmem, vmem, vmem),
        scratch_shapes=[
            pltpu.SMEM((1, 4), F32),
            pltpu.VMEM((LV, CC), F32),
            pltpu.VMEM((LV, CC), F32),
            pltpu.VMEM((LV, CC), F32),
            pltpu.VMEM((LV, 3 * CC), F32),
            pltpu.VMEM((1, 3 * CC), F32),
            pltpu.VMEM((1, 3 * CC), F32),
            pltpu.VMEM((1, CC), F32),
            pltpu.VMEM((NBK, 1, HB), jnp.int32),
            pltpu.VMEM((2, 3 * CC), jnp.int32),
            pltpu.VMEM((3, EXT, CC), F8),
            pltpu.VMEM((CC, HALO), F8),
            pltpu.VMEM((3, LV, CC), F32),
            pltpu.VMEM((3, 8, CC), F32),
            pltpu.VMEM((8, NBK, LV, HB), F32),
            pltpu.VMEM((8, NBK, LV, HB), F32),
            pltpu.VMEM((2, NBK, 1, HB), F32),
            pltpu.VMEM((2, NBK, 1, HB), F32),
            pltpu.VMEM((1, HB), F32),
            pltpu.VMEM((1, HB), F32),
            pltpu.VMEM((LINE, 1, HB), F32),
            pltpu.VMEM((n_all, 1, HB), F32),
            pltpu.VMEM((NBK, LV, HB), F32),
            pltpu.VMEM((n_mem, NBK, band, HB), F32),
            pltpu.VMEM((LV, CC), F32),
            pltpu.VMEM((n_mem, band, CC), F32),
            pltpu.VMEM((band, CC), F32),
            pltpu.VMEM((n_mem, band, CC), F32),
            dma((10,)),
            dma,
            dma((8,)),
            dma,
            dma((2,)),
            dma,
            dma,
            pltpu.SemaphoreType.REGULAR,
            dma,
            dma,
            dma,
            dma,
            dma((2,)),
            dma((2,)),
        ],
        compiler_params=pltpu.CompilerParams(collective_id=0, has_side_effects=True),
    )(
        model_parameters,
        acoustic_perturbation,
        prior_acoustic_state,
        thermal_anomaly,
        crossing_velocity,
        face_extent[None, :],
        face_metric_factor[None, :],
        reciprocal_polygon_surface[None, :],
        export_lists.reshape(NBK, 1, HB),
        face_neighbour_pair,
    )
    return pl.pallas_call(
        hand_over,
        out_shape=(
            jax.ShapeDtypeStruct((1, LV, CC), F32),
            jax.ShapeDtypeStruct((1, LV, CC), F32),
            jax.ShapeDtypeStruct((LV, CC), F32),
        ),
        in_specs=[vmem] * 3,
        out_specs=(anyw, anyw, anyw),
        scratch_shapes=[dma((3,))],
    )(*[pltpu.with_memory_space_constraint(x, pltpu.VMEM) for x in held])


def solution(mesh):
    in_specs = (
        P("member", None, "dom"),
        P("member", None, "dom"),
        P("member", None, "dom"),
        P("member", None),
        P(None, "dom"),
        P("dom"),
        P("dom"),
        P("dom"),
        P("dom"),
        P("dom", None, None),
        P(None, "dom"),
        P(None, "dom"),
    )
    out_specs = (P("member", None, "dom"), P("member", None, "dom"), P(None, "dom"))
    return jax.shard_map(
        per_device, mesh=mesh, in_specs=in_specs, out_specs=out_specs, check_vma=False
    )
```
